512 devices in a mesh: rows: 128 (over y_lo, x, z), cols: 4 (over y_hi, core).
Axes of the slice: x: 4, y: 4 (y_hi: 2, y_lo: 2; y = y_hi * 2 + y_lo), z: 16, core: 2. Of those that a mesh axis runs over, the one named last changes fastest.
Arguments:
- grad_out: bfloat16 [512, 512, 192], P(('rows', 'cols')), may hold values from -6 to 6
- inputs: bfloat16 [1024, 1024, 192], P('rows', 'cols'), may hold values from -6 to 6
- weight: bfloat16 [3, 3, 192, 192], replicated, may hold values from -0.15625 to 0.15625
Outputs:
- input_grad: bfloat16 [1024, 1024, 192], P('rows', 'cols')
- filter_grad: float32 [3, 3, 192, 192], replicated
The draws below stay inside these ranges and needn't reach their ends.
All inputs are finite; a program needn't handle non-finite values.
Results may differ from the reference program's by a relative error of at most 0.0028.
Values may be sent and summed in bfloat16 or wider, within the bound.
No kernel may reach another device: no remote copies, remote signals or barrier semaphores. Data moves between devices by JAX's collectives and lax.ppermute only.
A program may use at most 64 MiB of HBM per device.

```python
import jax
import jax.numpy as jnp
from jax import lax

C = 192
ROWS_DEV = 8
HEIGHT = 1024
WIDTH = 1024
POSITIONS = 262144


def steps_of(key, dims, cuts, least, largest):
    def one(dim, parts):
        draws = jax.random.uniform(jax.random.fold_in(jax.random.fold_in(key, 6), dim), (parts,), jnp.float32, least / len(cuts), largest / len(cuts))
        return jnp.repeat(jnp.exp(draws), dims[dim] // parts).reshape((-1,) + (1,) * (len(dims) - dim - 1))

    level = one(*cuts[0])
    for cut in cuts[1:]:
        level = level * one(*cut)
    return level


def bell_draw(rng, extent, scale, most, shards=(), kind=jnp.bfloat16):
    drawn = jax.random.normal(rng, extent, jnp.float32) * scale
    if len(shards) > 0:
        drawn = steps_of(rng, extent, shards, -0.22, 0.18) * drawn
    return jnp.clip(drawn, min=-most, max=most).astype(kind)


def setup_inputs(seed: int = 0) -> dict:
    key_of = jax.random.split(jax.random.key(seed), 4)
    return {
        "grad_out": bell_draw(key_of[0], (HEIGHT // 2, WIDTH // 2, C), 1.0, 6.0, ((0, 512),)),
        "inputs": bell_draw(key_of[1], (HEIGHT, WIDTH, C), 1.0, 6.0, ((0, 128), (1, 4))),
        "weight": bell_draw(key_of[2], (3, 3, C, C), (9 * C) ** -0.5, 0.15625),
    }


def tap_products(out_block, flat_weight):
    chans = flat_weight.shape[0]
    flat = out_block.reshape(-1, chans)
    products = jnp.dot(flat, flat_weight, preferred_element_type=jnp.float32)
    return products.reshape(out_block.shape[0], out_block.shape[1], 3, 3, chans)

def assemble(products, count_rows, count_cols):
    rows_even = products[:count_rows, :, 1]
    rows_odd = products[:count_rows, :, 2] + products[1:count_rows + 1, :, 0]

    def columns(mixed):
        even = mixed[:, :count_cols, 1]
        odd = mixed[:, :count_cols, 2] + mixed[:, 1:count_cols + 1, 0]
        return jnp.stack([even, odd], axis=2)
    placed = jnp.stack([columns(rows_even), columns(rows_odd)], axis=1)
    return placed.reshape(2 * count_rows, 2 * count_cols, products.shape[-1])

def filter_terms(input_band, out_band, row_taps):
    count_rows, count_cols, chans = out_band.shape
    split = input_band.reshape(count_rows + 1, 2, count_cols + 1, 2, chans)
    offsets = ((0, 0), (0, 1), (1, 0))
    pieces = []
    for row_tap in row_taps:
        start_row, parity_row = offsets[row_tap]
        for col_tap in range(3):
            start_col, parity_col = offsets[col_tap]
            pieces.append(split[start_row:start_row + count_rows, parity_row, start_col:start_col + count_cols, parity_col])
    stacked = jnp.stack(pieces, axis=2).reshape(count_rows * count_cols, len(pieces) * chans)
    flat_out = out_band.reshape(count_rows * count_cols, chans)
    return lax.dot_general(stacked, flat_out, (((0,), (0,)), ((), ())), preferred_element_type=jnp.float32)

def reference(grad_out, inputs, weight):
    half_rows, half_cols, chans = grad_out.shape
    band_rows = ROWS_DEV // 2
    flat_weight = jnp.transpose(weight, (3, 0, 1, 2)).reshape(chans, 9 * chans)
    padded_out = jnp.pad(grad_out, ((0, 1), (0, 1), (0, 0)))
    padded_in = jnp.pad(inputs, ((1, 1), (1, 1), (0, 0)))

    def step(total, index):
        start = (index * band_rows).astype(jnp.int32)
        out_block = lax.dynamic_slice_in_dim(padded_out, start, band_rows + 1, 0)
        input_band = lax.dynamic_slice_in_dim(padded_in, (2 * start).astype(jnp.int32), 2 * band_rows + 2, 0)
        block = assemble(tap_products(out_block, flat_weight), band_rows, half_cols).astype(jnp.bfloat16)
        terms = filter_terms(input_band, out_block[:band_rows, :half_cols], (0, 1, 2))
        return (total + terms, block)
    total, blocks = lax.scan(step, jnp.zeros((9 * chans, chans), jnp.float32), jnp.arange(half_rows // band_rows, dtype=jnp.int32))
    input_grad = blocks.reshape(2 * half_rows, 2 * half_cols, chans)
    filter_grad = total.reshape(3, 3, chans, chans) / jnp.sqrt(jnp.float32(POSITIONS))
    return (input_grad, filter_grad)
```

```python
import functools
import math

import jax
import jax.numpy as jnp
from jax import lax
from jax.experimental import pallas as pl
from jax.experimental.pallas import tpu as pltpu
from jax.sharding import Mesh
from jax.sharding import PartitionSpec as P

AXES = ("r0", "r1", "z1", "z0", "c0", "c1")
ROWS = ("r0", "r1", "z1", "z0")
COLS = ("c0", "c1")
NEAR = ("r0", "r1", "z0", "c0", "c1")
FAR = "z1"
BF = jnp.bfloat16
F32 = jnp.float32
LANES = 128
TOTAL = 3072
NT = (((1,), (1,)), ((), ()))
TN = (((0,), (0,)), ((), ()))
NN = (((1,), (0,)), ((), ()))


def mm(a, b, dims):
    return lax.dot_general(a, b, dims, preferred_element_type=F32)


def call(body, outs, flops, moved):
    return pl.pallas_call(
        body,
        out_shape=outs,
        cost_estimate=pl.CostEstimate(flops=flops, bytes_accessed=moved, transcendentals=0),
        compiler_params=pltpu.CompilerParams(vmem_limit_bytes=24 * 1024 * 1024),
    )


def split_matrix(width):
    half = width // 2
    q = lax.broadcasted_iota(jnp.int32, (width, width), 0)
    n = lax.broadcasted_iota(jnp.int32, (width, width), 1)
    source = jnp.where(n < half, 2 * n, 2 * (n - half) + 1)
    return jnp.where(q == source, 1.0, 0.0).astype(BF)


def send_body(grad_ref, last_ref, out_ref, row_ref):
    chans, width = grad_ref.shape
    blocks = out_ref.shape[0]
    block = width // blocks
    r = lax.broadcasted_iota(jnp.int32, (8, width), 0)
    q = lax.broadcasted_iota(jnp.int32, (8, width), 1)
    pick = jnp.where(q == (r + 1) * block, 1.0, 0.0).astype(BF)
    edge = mm(pick, grad_ref[...], NT)
    head = edge[:, :LANES].astype(BF)
    tail = jnp.concatenate([edge[:, LANES:], jnp.zeros((8, 2 * LANES - chans), F32)], axis=1).astype(BF)
    for d in range(blocks):
        out_ref[d, :chans, :] = grad_ref[:, d * block : (d + 1) * block]
        out_ref[d, chans:, :] = jnp.concatenate(
            [head[d : d + 1], tail[d : d + 1], jnp.zeros((6, LANES), BF)], axis=0
        )
    row_ref[...] = mm(last_ref[...], split_matrix(2 * LANES), NN).astype(BF)


def split_body(in_ref, out_ref):
    rows, chans, width = in_ref.shape
    flat = in_ref[...].reshape(rows * chans, width)
    out_ref[...] = mm(flat, split_matrix(width), NN).astype(BF).reshape(rows, chans, width)


def shifted(grads, edges):
    q = lax.broadcasted_iota(jnp.int32, (LANES, LANES), 0)
    n = lax.broadcasted_iota(jnp.int32, (LANES, LANES), 1)
    move = jnp.where(q == n + 1, 1.0, 0.0).astype(BF)
    r = lax.broadcasted_iota(jnp.int32, (8, LANES), 0)
    lane = lax.broadcasted_iota(jnp.int32, (8, LANES), 1)
    out = []
    for k, block in enumerate(grads):
        place = jnp.where((r == k) & (lane == LANES - 1), 1.0, 0.0).astype(BF)
        out.append((mm(block, move, NN) + mm(edges, place, TN)).astype(BF))
    return out


def edges_of(blocks, chans):
    rows = [jnp.concatenate([b[chans : chans + 1, :], b[chans + 1 : chans + 2, : chans - LANES]], axis=1) for b in blocks]
    rows.append(jnp.zeros((8 - len(rows), chans), BF))
    return jnp.concatenate(rows, axis=0)


def filter_body(got_ref, split_ref, above_ref, out_ref):
    rows, chans, width = split_ref.shape
    half = rows // 2
    blocks = [got_ref[k] for k in range(half)]
    grads = [b[:chans, :] for b in blocks]
    moved = shifted(grads, edges_of(blocks, chans))
    spare = jnp.zeros((2 * LANES - chans, half * LANES), BF)
    here = jnp.concatenate([jnp.concatenate(grads, axis=1), spare], axis=0)
    right = jnp.concatenate([jnp.concatenate(moved, axis=1), spare], axis=0)

    def line(p, odd):
        cut = slice(LANES, 2 * LANES) if odd else slice(0, LANES)
        return above_ref[:, cut] if p < 0 else split_ref[p, :, cut]

    step = chans + chans // 2
    for a in range(3):
        for b in range(3):
            left = jnp.concatenate([line(2 * k + a - 1, b != 1) for k in range(half)], axis=1)
            term = mm(left, right if b == 0 else here, NT)
            base = (3 * a + b) * step
            far = term[:, LANES:]
            packed = far[: chans // 2] + pltpu.roll(far[chans // 2 :], LANES // 2, 1)
            out_ref[base : base + chans, :] = term[:, :LANES].astype(BF)
            out_ref[base + chans : base + step, :] = packed.astype(BF)
    out_ref[9 * step :, :] = jnp.zeros((TOTAL - 9 * step, LANES), BF)


def near_body(in_ref, out_ref):
    total = jnp.sum(in_ref[...].astype(F32), axis=0)
    out_ref[...] = jnp.broadcast_to(total[None], out_ref.shape)


def far_body(in_ref, out_ref):
    total = jnp.sum(in_ref[...], axis=0).astype(BF)
    out_ref[...] = jnp.broadcast_to(total[None], out_ref.shape)


def unpack_body(scale, in_ref, out_ref):
    chans = out_ref.shape[-1]
    step = chans + chans // 2
    for t in range(9):
        base = t * step
        near = in_ref[base : base + chans, :].astype(F32) * scale
        far = in_ref[base + chans : base + step, :].astype(F32) * scale
        out_ref[t, :, :LANES] = near
        out_ref[t, : chans // 2, LANES:] = far[:, : LANES // 2]
        out_ref[t, chans // 2 :, LANES:] = pltpu.roll(far, LANES // 2, 1)[:, : LANES // 2]


def input_body(got_ref, below_ref, weight_ref, out_ref):
    rows, chans, width = out_ref.shape
    half = rows // 2
    blocks = [got_ref[k] for k in range(half)] + [below_ref[...]]
    grads = [b[:chans, :] for b in blocks]
    moved = shifted(grads, edges_of(blocks, chans))
    here = jnp.concatenate(grads[:half], axis=1)
    right = jnp.concatenate(moved[:half], axis=1)
    here_down = jnp.concatenate(grads[1:], axis=1)
    right_down = jnp.concatenate(moved[1:], axis=1)

    def tap(a, b, g):
        return mm(weight_ref[a, b], g, NN)

    even_even = tap(1, 1, here)
    even_odd = tap(1, 2, here) + tap(1, 0, right)
    odd_even = tap(2, 1, here) + tap(0, 1, here_down)
    odd_odd = tap(2, 2, here) + tap(2, 0, right) + tap(0, 2, here_down) + tap(0, 0, right_down)
    q = lax.broadcasted_iota(jnp.int32, (width, width), 1)
    n = lax.broadcasted_iota(jnp.int32, (width, width), 0)
    target = jnp.where(n < LANES, 2 * n, 2 * (n - LANES) + 1)
    merge = jnp.where(q == target, 1.0, 0.0).astype(BF)
    for k in range(half):
        cut = slice(k * LANES, (k + 1) * LANES)
        for p, left, odd in ((2 * k, even_even, even_odd), (2 * k + 1, odd_even, odd_odd)):
            both = jnp.concatenate([left[:, cut], odd[:, cut]], axis=1).astype(BF)
            out_ref[p] = mm(both, merge, NN).astype(BF)


def shape(dims, dtype):
    return jax.ShapeDtypeStruct(dims, dtype)


def moved_rows(x, by):
    devices = lax.axis_size(ROWS)
    pairs = [(i, i + by) for i in range(devices) if 0 <= i + by < devices]
    return lax.ppermute(x, ROWS, pairs)


def swap(x, axes):
    return lax.all_to_all(x, axes, split_axis=0, concat_axis=0, tiled=True)


def per_device(grad_out, inputs, weight):
    chans = weight.shape[2]
    rows, cols = inputs.shape[:2]
    half = rows // 2
    groups = lax.axis_size(COLS)
    near, far = lax.axis_size(NEAR), lax.axis_size(FAR)
    chunk = TOTAL // near
    message = chans + 8
    positions = half * lax.axis_size(ROWS) * (cols // 2) * groups
    grad = jnp.transpose(grad_out, (0, 2, 1))[0]
    lines = jnp.transpose(inputs, (0, 2, 1))

    sent, last = call(
        send_body,
        (shape((groups, message, LANES), BF), shape((chans, cols), BF)),
        10**8,
        10**6,
    )(grad, lines[rows - 1])
    above = moved_rows(last, 1)
    got = swap(sent, COLS)
    split = call(split_body, shape((rows, chans, cols), BF), 2 * 10**8, 16 * 10**5)(lines)
    terms = call(filter_body, shape((TOTAL, LANES), BF), 10**9, 2 * 10**6)(got, split, above)
    below = moved_rows(got[0], -1)
    part = swap(terms.reshape(near, chunk, LANES), NEAR)
    input_grad = call(input_body, shape((rows, chans, cols), BF), 10**9, 2 * 10**6)(got, below, weight)
    part = call(near_body, shape((far, chunk, LANES), F32), 10**6, 10**6)(part)
    part = swap(part, FAR)
    part = call(far_body, shape((near, chunk, LANES), BF), 10**6, 10**6)(part)
    whole = swap(part, NEAR).reshape(TOTAL, LANES)
    filter_grad = call(
        functools.partial(unpack_body, 1.0 / math.sqrt(positions)), shape((9, chans, chans), F32), 10**6, 2 * 10**6
    )(whole)
    return (jnp.transpose(input_grad, (0, 2, 1)), filter_grad.reshape(3, 3, chans, chans))


def solution(mesh):
    split = Mesh(mesh.devices.reshape(2, 4, 8, 2, 2, 2), AXES)
    return build(split)


def build(split):
    return jax.shard_map(
        per_device,
        mesh=split,
        in_specs=(P(ROWS + COLS, None, None), P(ROWS, COLS, None), P()),
        out_specs=(P(ROWS, COLS, None), P()),
        check_vma=False,
    )
```

```python
import functools
import math

import jax
import jax.numpy as jnp
from jax import lax
from jax.experimental import pallas as pl
from jax.experimental.pallas import tpu as pltpu
from jax.sharding import Mesh
from jax.sharding import PartitionSpec as P

AXES = ("r0", "r1", "z1", "z0", "c0", "c1")
ROWS = ("r0", "r1", "z1", "z0")
COLS = ("c0", "c1")
NEAR = ("r0", "r1", "z0", "c0", "c1")
FAR = "z1"
BF = jnp.bfloat16
F32 = jnp.float32
LANES = 128
TOTAL = 3072
NT = (((1,), (1,)), ((), ()))
TN = (((0,), (0,)), ((), ()))
NN = (((1,), (0,)), ((), ()))


def mm(a, b, dims):
    return lax.dot_general(a, b, dims, preferred_element_type=F32)


def call(body, outs, flops, moved):
    return pl.pallas_call(
        body,
        out_shape=outs,
        cost_estimate=pl.CostEstimate(flops=flops, bytes_accessed=moved, transcendentals=0),
        compiler_params=pltpu.CompilerParams(vmem_limit_bytes=24 * 1024 * 1024),
    )


def split_matrix(width):
    half = width // 2
    q = lax.broadcasted_iota(jnp.int32, (width, width), 0)
    n = lax.broadcasted_iota(jnp.int32, (width, width), 1)
    source = jnp.where(n < half, 2 * n, 2 * (n - half) + 1)
    return jnp.where(q == source, 1.0, 0.0).astype(BF)


def send_body(grad_ref, lines_ref, out_ref, row_ref, grad, last, edges, in_sem, out_sem):
    chans, width = grad_ref.shape
    blocks = out_ref.shape[0]
    block = width // blocks
    take_grad = pltpu.make_async_copy(grad_ref, grad, in_sem.at[0])
    take_last = pltpu.make_async_copy(lines_ref.at[lines_ref.shape[0] - 1], last, in_sem.at[1])
    take_grad.start()
    take_last.start()
    take_grad.wait()
    puts = []
    for d in range(blocks):
        put = pltpu.make_async_copy(
            grad.at[:, d * block : (d + 1) * block], out_ref.at[d, pl.ds(0, chans), :], out_sem.at[d]
        )
        put.start()
        puts.append(put)
    r = lax.broadcasted_iota(jnp.int32, (8, width), 0)
    q = lax.broadcasted_iota(jnp.int32, (8, width), 1)
    pick = jnp.where(q == (r + 1) * block, 1.0, 0.0).astype(BF)
    edge = mm(pick, grad[...], NT)
    head = edge[:, :LANES]
    tail = jnp.concatenate([edge[:, LANES:], jnp.zeros((8, 2 * LANES - chans), F32)], axis=1)
    for d in range(blocks):
        edges[d] = jnp.concatenate([head[d : d + 1], tail[d : d + 1], jnp.zeros((6, LANES), F32)], axis=0).astype(BF)
    put = pltpu.make_async_copy(edges, out_ref.at[:, pl.ds(chans, 8), :], out_sem.at[blocks])
    put.start()
    puts.append(put)
    take_last.wait()
    row_ref[...] = mm(last[...], split_matrix(2 * LANES), NN).astype(BF)
    for put in puts:
        put.wait()


def split_body(in_ref, out_ref):
    rows, chans, width = in_ref.shape
    flat = in_ref[...].reshape(rows * chans, width)
    out_ref[...] = mm(flat, split_matrix(width), NN).astype(BF).reshape(rows, chans, width)


def shifted(grads, edges):
    q = lax.broadcasted_iota(jnp.int32, (LANES, LANES), 0)
    n = lax.broadcasted_iota(jnp.int32, (LANES, LANES), 1)
    move = jnp.where(q == n + 1, 1.0, 0.0).astype(BF)
    r = lax.broadcasted_iota(jnp.int32, (8, LANES), 0)
    lane = lax.broadcasted_iota(jnp.int32, (8, LANES), 1)
    out = []
    for k, block in enumerate(grads):
        place = jnp.where((r == k) & (lane == LANES - 1), 1.0, 0.0).astype(BF)
        out.append((mm(block, move, NN) + mm(edges, place, TN)).astype(BF))
    return out


def edges_of(blocks, chans):
    rows = [jnp.concatenate([b[chans : chans + 1, :], b[chans + 1 : chans + 2, : chans - LANES]], axis=1) for b in blocks]
    rows.append(jnp.zeros((8 - len(rows), chans), BF))
    return jnp.concatenate(rows, axis=0)


def filter_body(got_ref, split_ref, above_ref, out_ref):
    rows, chans, width = split_ref.shape
    half = rows // 2
    blocks = [got_ref[k] for k in range(half)]
    grads = [b[:chans, :] for b in blocks]
    moved = shifted(grads, edges_of(blocks, chans))
    spare = jnp.zeros((2 * LANES - chans, half * LANES), BF)
    here = jnp.concatenate([jnp.concatenate(grads, axis=1), spare], axis=0)
    right = jnp.concatenate([jnp.concatenate(moved, axis=1), spare], axis=0)

    def line(p, odd):
        cut = slice(LANES, 2 * LANES) if odd else slice(0, LANES)
        return above_ref[:, cut] if p < 0 else split_ref[p, :, cut]

    step = chans + chans // 2
    for a in range(3):
        for b in range(3):
            left = jnp.concatenate([line(2 * k + a - 1, b != 1) for k in range(half)], axis=1)
            term = mm(left, right if b == 0 else here, NT)
            base = (3 * a + b) * step
            far = term[:, LANES:]
            packed = far[: chans // 2] + pltpu.roll(far[chans // 2 :], LANES // 2, 1)
            out_ref[base : base + chans, :] = term[:, :LANES].astype(BF)
            out_ref[base + chans : base + step, :] = packed.astype(BF)
    out_ref[9 * step :, :] = jnp.zeros((TOTAL - 9 * step, LANES), BF)


def near_body(in_ref, out_ref):
    total = jnp.sum(in_ref[...].astype(F32), axis=0)
    out_ref[...] = jnp.broadcast_to(total[None], out_ref.shape)


def far_body(in_ref, out_ref):
    total = jnp.sum(in_ref[...], axis=0).astype(BF)
    out_ref[...] = jnp.broadcast_to(total[None], out_ref.shape)


def unpack_body(scale, in_ref, out_ref):
    chans = out_ref.shape[-1]
    step = chans + chans // 2
    for t in range(9):
        base = t * step
        near = in_ref[base : base + chans, :].astype(F32) * scale
        far = in_ref[base + chans : base + step, :].astype(F32) * scale
        out_ref[t, :, :LANES] = near
        out_ref[t, : chans // 2, LANES:] = far[:, : LANES // 2]
        out_ref[t, chans // 2 :, LANES:] = pltpu.roll(far, LANES // 2, 1)[:, : LANES // 2]


def input_body(got_ref, below_ref, weight_ref, out_ref):
    rows, chans, width = out_ref.shape
    half = rows // 2
    blocks = [got_ref[k] for k in range(half)] + [below_ref[...]]
    grads = [b[:chans, :] for b in blocks]
    moved = shifted(grads, edges_of(blocks, chans))
    here = jnp.concatenate(grads[:half], axis=1)
    right = jnp.concatenate(moved[:half], axis=1)
    here_down = jnp.concatenate(grads[1:], axis=1)
    right_down = jnp.concatenate(moved[1:], axis=1)

    def tap(a, b, g):
        return mm(weight_ref[a, b], g, NN)

    even_even = tap(1, 1, here)
    even_odd = tap(1, 2, here) + tap(1, 0, right)
    odd_even = tap(2, 1, here) + tap(0, 1, here_down)
    odd_odd = tap(2, 2, here) + tap(2, 0, right) + tap(0, 2, here_down) + tap(0, 0, right_down)
    q = lax.broadcasted_iota(jnp.int32, (width, width), 1)
    n = lax.broadcasted_iota(jnp.int32, (width, width), 0)
    target = jnp.where(n < LANES, 2 * n, 2 * (n - LANES) + 1)
    merge = jnp.where(q == target, 1.0, 0.0).astype(BF)
    for k in range(half):
        cut = slice(k * LANES, (k + 1) * LANES)
        for p, left, odd in ((2 * k, even_even, even_odd), (2 * k + 1, odd_even, odd_odd)):
            both = jnp.concatenate([left[:, cut], odd[:, cut]], axis=1).astype(BF)
            out_ref[p] = mm(both, merge, NN).astype(BF)


def shape(dims, dtype):
    return jax.ShapeDtypeStruct(dims, dtype)


def moved_rows(x, by):
    devices = lax.axis_size(ROWS)
    pairs = [(i, i + by) for i in range(devices) if 0 <= i + by < devices]
    return lax.ppermute(x, ROWS, pairs)


def swap(x, axes):
    return lax.all_to_all(x, axes, split_axis=0, concat_axis=0, tiled=True)


def per_device(grad_out, inputs, weight):
    chans = weight.shape[2]
    rows, cols = inputs.shape[:2]
    half = rows // 2
    groups = lax.axis_size(COLS)
    near, far = lax.axis_size(NEAR), lax.axis_size(FAR)
    chunk = TOTAL // near
    message = chans + 8
    positions = half * lax.axis_size(ROWS) * (cols // 2) * groups
    grad = jnp.transpose(grad_out, (0, 2, 1))[0]
    lines = jnp.transpose(inputs, (0, 2, 1))

    far_memory = pl.BlockSpec(memory_space=pltpu.HBM)
    sent, last = pl.pallas_call(
        send_body,
        out_shape=(shape((groups, message, LANES), BF), shape((chans, cols), BF)),
        in_specs=[far_memory, far_memory],
        out_specs=(far_memory, pl.BlockSpec((chans, cols), lambda: (0, 0))),
        scratch_shapes=[
            pltpu.VMEM((chans, groups * LANES), BF),
            pltpu.VMEM((chans, cols), BF),
            pltpu.VMEM((groups, 8, LANES), BF),
            pltpu.SemaphoreType.DMA((2,)),
            pltpu.SemaphoreType.DMA((groups + 1,)),
        ],
        cost_estimate=pl.CostEstimate(flops=10**8, bytes_accessed=10**6, transcendentals=0),
    )(grad, lines)
    above = moved_rows(last, 1)
    got = swap(sent, COLS)
    split = call(split_body, shape((rows, chans, cols), BF), 2 * 10**8, 16 * 10**5)(lines)
    terms = call(filter_body, shape((TOTAL, LANES), BF), 10**9, 2 * 10**6)(got, split, above)
    below = moved_rows(got[0], -1)
    part = swap(terms.reshape(near, chunk, LANES), NEAR)
    input_grad = call(input_body, shape((rows, chans, cols), BF), 10**9, 2 * 10**6)(got, below, weight)
    part, input_grad = lax.optimization_barrier((part, input_grad))
    part = call(near_body, shape((far, chunk, LANES), F32), 10**6, 10**6)(part)
    part = swap(part, FAR)
    part = call(far_body, shape((near, chunk, LANES), BF), 10**6, 10**6)(part)
    whole = swap(part, NEAR).reshape(TOTAL, LANES)
    filter_grad = call(
        functools.partial(unpack_body, 1.0 / math.sqrt(positions)), shape((9, chans, chans), F32), 10**6, 2 * 10**6
    )(whole)
    return (jnp.transpose(input_grad, (0, 2, 1)), filter_grad.reshape(3, 3, chans, chans))


def solution(mesh):
    split = Mesh(mesh.devices.reshape(2, 4, 8, 2, 2, 2), AXES)
    return build(split)


def build(split):
    return jax.shard_map(
        per_device,
        mesh=split,
        in_specs=(P(ROWS + COLS, None, None), P(ROWS, COLS, None), P()),
        out_specs=(P(ROWS, COLS, None), P()),
        check_vma=False,
    )
```

```python
import functools
import math

import jax
import jax.numpy as jnp
from jax import lax
from jax.experimental import pallas as pl
from jax.experimental.pallas import tpu as pltpu
from jax.sharding import Mesh
from jax.sharding import PartitionSpec as P

AXES = ("r0", "r1", "z1", "z0", "c0", "c1")
ROWS = ("r0", "r1", "z1", "z0")
COLS = ("c0", "c1")
NEAR = ("r0", "r1", "z0", "c0")
FAR = "z1"
CORE = "c1"
BF = jnp.bfloat16
F32 = jnp.float32
LANES = 128
TOTAL = 3072
NT = (((1,), (1,)), ((), ()))
STEPS = 32256.0
SMALLEST = 2.0**-126
NN = (((1,), (0,)), ((), ()))


def mm(a, b, dims):
    return lax.dot_general(a, b, dims, preferred_element_type=F32)


def call(body, outs, flops, moved):
    return pl.pallas_call(
        body,
        out_shape=outs,
        cost_estimate=pl.CostEstimate(flops=flops, bytes_accessed=moved, transcendentals=0),
        compiler_params=pltpu.CompilerParams(vmem_limit_bytes=24 * 1024 * 1024),
    )


def split_matrix(width):
    half = width // 2
    q = lax.broadcasted_iota(jnp.int32, (width, width), 0)
    n = lax.broadcasted_iota(jnp.int32, (width, width), 1)
    source = jnp.where(n < half, 2 * n, 2 * (n - half) + 1)
    return jnp.where(q == source, 1.0, 0.0).astype(BF)


def move_matrix(last):
    q = lax.broadcasted_iota(jnp.int32, (2 * LANES, LANES), 0)
    n = lax.broadcasted_iota(jnp.int32, (2 * LANES, LANES), 1)
    keep = (q == n + 1) & ((q < LANES) | jnp.logical_not(last))
    return jnp.where(keep, 1.0, 0.0).astype(BF)


def filter_body(got_ref, lines_ref, above_ref, out_ref, pair_ref):
    rows, chans, width = lines_ref.shape
    half = rows // 2
    groups = lax.axis_size(COLS)
    mine = lax.axis_index(COLS)
    here_at = pl.multiple_of(mine * LANES, LANES)
    next_at = pl.multiple_of(jnp.minimum(mine + 1, groups - 1) * LANES, LANES)
    move = move_matrix(jnp.broadcast_to(mine, (2 * LANES, LANES)) == groups - 1)
    cut = split_matrix(width)
    grads, moved = [], []
    for k in range(half):
        block = got_ref[k, :, pl.ds(here_at, LANES)]
        after = got_ref[k, :, pl.ds(next_at, LANES)]
        grads.append(block)
        moved.append(mm(jnp.concatenate([block, after], axis=1), move, NN).astype(BF))
        pair_ref[k, 0] = block
        pair_ref[k, 1] = moved[-1]
    flat = mm(lines_ref[...].reshape(rows * chans, width), cut, NN).astype(BF)
    top = mm(above_ref[...], cut, NN).astype(BF)
    spare = jnp.zeros((2 * LANES - chans, half * LANES), BF)
    here = jnp.concatenate([jnp.concatenate(grads, axis=1), spare], axis=0)
    right = jnp.concatenate([jnp.concatenate(moved, axis=1), spare], axis=0)

    def line(p, odd):
        lanes = slice(LANES, 2 * LANES) if odd else slice(0, LANES)
        return top[:, lanes] if p < 0 else flat[p * chans : (p + 1) * chans, lanes]

    step = chans + chans // 2
    for a in range(3):
        for b in range(3):
            left = jnp.concatenate([line(2 * k + a - 1, b != 1) for k in range(half)], axis=1)
            term = mm(left, right if b == 0 else here, NT)
            base = (3 * a + b) * step
            far = term[:, LANES:]
            out_ref[base : base + chans, :] = term[:, :LANES]
            out_ref[base + chans : base + step, :] = far[: chans // 2] + pltpu.roll(far[chans // 2 :], LANES // 2, 1)
    out_ref[9 * step :, :] = jnp.zeros((TOTAL - 9 * step, LANES), F32)


def pair_body(in_ref, out_ref):
    out_ref[...] = (in_ref[0] + in_ref[1]).astype(BF)


def coded(value, top):
    count = jnp.floor(jnp.abs(value) * (STEPS / top) + 0.5)
    power = jnp.floor(count * (1.0 / 128.0))
    rest = count - 128.0 * power
    code = (1.0 + rest * (1.0 / 128.0)) * SMALLEST
    power = power.astype(jnp.int32)
    for bit in (0, 1, 2, 3, 4, 5, 6, 7, 7):
        code = jnp.where((power & (1 << bit)) != 0, code * 2.0 ** min(1 << bit, 64), code)
    return jnp.where(value < 0, -code, code).astype(BF)


def decoded(code, top):
    code = code.astype(F32)
    size = jnp.abs(code)
    big = size >= 4.0
    power = jnp.where(big, 128.0, 0.0)
    for _ in range(2):
        size = jnp.where(big, size * 2.0**-64, size)
    for bit in range(6, -1, -1):
        span = float(1 << bit)
        big = size >= SMALLEST * 2.0**span
        size = jnp.where(big, size * 2.0**-span, size)
        power = jnp.where(big, power + span, power)
    count = 128.0 * power + (size * (1.0 / SMALLEST) - 1.0) * 128.0
    return jnp.where(code < 0, -count, count) * (top * (1.0 / STEPS))


def near_body(in_ref, out_ref):
    total = jnp.sum(in_ref[...].astype(F32), axis=0)
    chunk = total.shape[0]
    top = jnp.max(jnp.max(jnp.abs(total), axis=0, keepdims=True), axis=1, keepdims=True)
    top = jnp.maximum(top * 1.0078125, 1e-30).astype(BF)
    code = coded(total, top.astype(F32))
    head = jnp.broadcast_to(top, (8, LANES))
    for k in range(out_ref.shape[0]):
        out_ref[k, :chunk, :] = code
        out_ref[k, chunk:, :] = head


def far_body(in_ref, out_ref):
    chunk = out_ref.shape[1]
    total = None
    for k in range(in_ref.shape[0]):
        top = in_ref[k, chunk:, :].astype(F32)[:1]
        term = decoded(in_ref[k, :chunk, :], top)
        total = term if total is None else total + term
    out_ref[...] = jnp.broadcast_to(total.astype(BF)[None], out_ref.shape)


def unpack_body(scale, in_ref, out_ref):
    chans = out_ref.shape[-1]
    step = chans + chans // 2
    for t in range(9):
        base = t * step
        near = in_ref[base : base + chans, :].astype(F32) * scale
        far = in_ref[base + chans : base + step, :].astype(F32) * scale
        out_ref[t, :, :LANES] = near
        out_ref[t, : chans // 2, LANES:] = far[:, : LANES // 2]
        out_ref[t, chans // 2 :, LANES:] = pltpu.roll(far, LANES // 2, 1)[:, : LANES // 2]


def input_body(pair_ref, below_ref, weight_ref, out_ref):
    rows, chans, width = out_ref.shape
    half = rows // 2
    grads = [pair_ref[k, 0] for k in range(half)] + [below_ref[0]]
    moved = [pair_ref[k, 1] for k in range(half)] + [below_ref[1]]
    here = jnp.concatenate(grads[:half], axis=1)
    right = jnp.concatenate(moved[:half], axis=1)
    here_down = jnp.concatenate(grads[1:], axis=1)
    right_down = jnp.concatenate(moved[1:], axis=1)

    def tap(a, b, g):
        return mm(weight_ref[a, b], g, NN)

    even_even = tap(1, 1, here)
    even_odd = tap(1, 2, here) + tap(1, 0, right)
    odd_even = tap(2, 1, here) + tap(0, 1, here_down)
    odd_odd = tap(2, 2, here) + tap(2, 0, right) + tap(0, 2, here_down) + tap(0, 0, right_down)
    q = lax.broadcasted_iota(jnp.int32, (width, width), 1)
    n = lax.broadcasted_iota(jnp.int32, (width, width), 0)
    target = jnp.where(n < LANES, 2 * n, 2 * (n - LANES) + 1)
    merge = jnp.where(q == target, 1.0, 0.0).astype(BF)
    for k in range(half):
        cut = slice(k * LANES, (k + 1) * LANES)
        for p, left, odd in ((2 * k, even_even, even_odd), (2 * k + 1, odd_even, odd_odd)):
            both = jnp.concatenate([left[:, cut], odd[:, cut]], axis=1).astype(BF)
            out_ref[p] = mm(both, merge, NN).astype(BF)


def shape(dims, dtype):
    return jax.ShapeDtypeStruct(dims, dtype)


def moved_rows(x, by):
    devices = lax.axis_size(ROWS)
    pairs = [(i, i + by) for i in range(devices) if 0 <= i + by < devices]
    return lax.ppermute(x, ROWS, pairs)


def swap(x, axes):
    return lax.all_to_all(x, axes, split_axis=0, concat_axis=0, tiled=True)


def per_device(grad_out, inputs, weight):
    chans = weight.shape[2]
    rows, cols = inputs.shape[:2]
    half = rows // 2
    near, far = lax.axis_size(NEAR), lax.axis_size(FAR)
    own = TOTAL // lax.axis_size(CORE)
    chunk = own // near
    positions = half * lax.axis_size(ROWS) * (cols // 2) * lax.axis_size(COLS)
    grad = jnp.transpose(grad_out, (0, 2, 1))
    lines = jnp.transpose(inputs, (0, 2, 1))

    above = moved_rows(lines[rows - 1], 1)
    got = lax.all_gather(grad, COLS, axis=0, tiled=True)
    terms, pairs = call(
        filter_body,
        (shape((TOTAL, LANES), F32), shape((half, 2, chans, LANES), BF)),
        10**9,
        4 * 10**6,
    )(got, lines, above)
    part = swap(terms.reshape(2, own, LANES), CORE)
    part = call(pair_body, shape((own, LANES), BF), 10**6, 2 * 10**6)(part)
    part = swap(part.reshape(near, chunk, LANES), NEAR)
    part, pairs = lax.optimization_barrier((part, pairs))
    below = moved_rows(pairs[0], -1)
    part = call(near_body, shape((far, chunk + 8, LANES), BF), 10**6, 10**6)(part)
    part = swap(part, FAR)
    input_grad = call(input_body, shape((rows, chans, cols), BF), 10**9, 2 * 10**6)(pairs, below, weight)
    part, input_grad = lax.optimization_barrier((part, input_grad))
    part = call(far_body, shape((near, chunk, LANES), BF), 10**6, 10**6)(part)
    part = swap(part, NEAR).reshape(own, LANES)
    whole = lax.all_gather(part, CORE, axis=0, tiled=True)
    filter_grad = call(
        functools.partial(unpack_body, 1.0 / math.sqrt(positions)), shape((9, chans, chans), F32), 10**6, 2 * 10**6
    )(whole)
    return (jnp.transpose(input_grad, (0, 2, 1)), filter_grad.reshape(3, 3, chans, chans))


def solution(mesh):
    split = Mesh(mesh.devices.reshape(2, 4, 8, 2, 2, 2), AXES)
    return build(split)


def build(split):
    return jax.shard_map(
        per_device,
        mesh=split,
        in_specs=(P(ROWS + COLS, None, None), P(ROWS, COLS, None), P()),
        out_specs=(P(ROWS, COLS, None), P()),
        check_vma=False,
    )
```

```python
import functools
import math

import jax
import jax.numpy as jnp
from jax import lax
from jax.experimental import pallas as pl
from jax.experimental.pallas import tpu as pltpu
from jax.sharding import Mesh
from jax.sharding import PartitionSpec as P


AXES = ("r0", "r1", "z1", "z0", "c0", "c1")
ROWS = ("r0", "r1", "z1", "z0")
COLS = ("c0", "c1")
NEAR = ("r0", "r1", "z0", "c0")
FAR = "z1"
CORE = "c1"
BF = jnp.bfloat16
F32 = jnp.float32
LANES = 128
TOTAL = 3072
NT = (((1,), (1,)), ((), ()))
TN = (((0,), (0,)), ((), ()))
STEPS = 32256.0
SMALLEST = 2.0**-126
NN = (((1,), (0,)), ((), ()))


def mm(a, b, dims):
    return lax.dot_general(a, b, dims, preferred_element_type=F32)


def call(body, outs, flops, moved):
    return pl.pallas_call(
        body,
        out_shape=outs,
        cost_estimate=pl.CostEstimate(flops=flops, bytes_accessed=moved, transcendentals=0),
        compiler_params=pltpu.CompilerParams(vmem_limit_bytes=24 * 1024 * 1024),
    )


def split_matrix(width):
    half = width // 2
    q = lax.broadcasted_iota(jnp.int32, (width, width), 0)
    n = lax.broadcasted_iota(jnp.int32, (width, width), 1)
    source = jnp.where(n < half, 2 * n, 2 * (n - half) + 1)
    return jnp.where(q == source, 1.0, 0.0).astype(BF)


def send_body(grad_ref, out_ref):
    chans, width = grad_ref.shape
    blocks = out_ref.shape[0]
    block = width // blocks
    r = lax.broadcasted_iota(jnp.int32, (8, width), 0)
    q = lax.broadcasted_iota(jnp.int32, (8, width), 1)
    pick = jnp.where(q == (r + 1) * block, 1.0, 0.0).astype(BF)
    edge = mm(pick, grad_ref[...], NT)
    head = edge[:, :LANES].astype(BF)
    tail = jnp.concatenate([edge[:, LANES:], jnp.zeros((8, 2 * LANES - chans), F32)], axis=1).astype(BF)
    for d in range(blocks):
        out_ref[d, :chans, :] = grad_ref[:, d * block : (d + 1) * block]
        out_ref[d, chans:, :] = jnp.concatenate(
            [head[d : d + 1], tail[d : d + 1], jnp.zeros((6, LANES), BF)], axis=0
        )


def split_body(lines_ref, row_ref, split_ref):
    rows, chans, width = lines_ref.shape
    flat = lines_ref[...].reshape(rows * chans, width)
    flat = mm(flat, split_matrix(width), NN).astype(BF).reshape(rows, chans, width)
    split_ref[...] = flat
    row_ref[...] = flat[rows - 1]


def shifted(grads, edges):
    q = lax.broadcasted_iota(jnp.int32, (LANES, LANES), 0)
    n = lax.broadcasted_iota(jnp.int32, (LANES, LANES), 1)
    move = jnp.where(q == n + 1, 1.0, 0.0).astype(BF)
    r = lax.broadcasted_iota(jnp.int32, (8, LANES), 0)
    lane = lax.broadcasted_iota(jnp.int32, (8, LANES), 1)
    out = []
    for k, block in enumerate(grads):
        place = jnp.where((r == k) & (lane == LANES - 1), 1.0, 0.0).astype(BF)
        out.append((mm(block, move, NN) + mm(edges, place, TN)).astype(BF))
    return out


def edges_of(blocks, chans):
    rows = [jnp.concatenate([b[chans : chans + 1, :], b[chans + 1 : chans + 2, : chans - LANES]], axis=1) for b in blocks]
    rows.append(jnp.zeros((8 - len(rows), chans), BF))
    return jnp.concatenate(rows, axis=0)


def filter_body(got_ref, split_ref, above_ref, out_ref, pair_ref):
    rows, chans, _ = split_ref.shape
    half = rows // 2
    mine = lax.axis_index(CORE)
    blocks = [got_ref[k] for k in range(half)]
    grads = [b[:chans, :] for b in blocks]
    moved = shifted(grads, edges_of(blocks, chans))
    for k in range(half):
        pair_ref[k, 0] = grads[k]
        pair_ref[k, 1] = moved[k]
    spare = jnp.zeros((2 * LANES - chans, half * LANES), BF)
    here = jnp.concatenate([jnp.concatenate(grads, axis=1), spare], axis=0)
    right = jnp.concatenate([jnp.concatenate(moved, axis=1), spare], axis=0)

    def line(p, odd):
        lanes = slice(LANES, 2 * LANES) if odd else slice(0, LANES)
        return above_ref[:, lanes] if p < 0 else split_ref[p, :, lanes]

    own = out_ref.shape[1]

    def put(base, value):
        count = value.shape[0]
        for core in range(2):
            low, high = max(base, core * own), min(base + count, (core + 1) * own)
            if low < high:
                out_ref[mine ^ core, low - core * own : high - core * own, :] = value[low - base : high - base]

    step = chans + chans // 2
    for a in range(3):
        for b in range(3):
            left = jnp.concatenate([line(2 * k + a - 1, b != 1) for k in range(half)], axis=1)
            term = mm(left, right if b == 0 else here, NT)
            base = (3 * a + b) * step
            far = term[:, LANES:]
            put(base, term[:, :LANES])
            put(base + chans, far[: chans // 2] + pltpu.roll(far[chans // 2 :], LANES // 2, 1))
    put(9 * step, jnp.zeros((TOTAL - 9 * step, LANES), F32))


def pair_body(mine_ref, other_ref, out_ref):
    out_ref[...] = (mine_ref[0] + other_ref[...]).astype(BF)


def coded(value, top):
    count = jnp.floor(jnp.abs(value) * (STEPS / top) + 0.5)
    power = jnp.floor(count * (1.0 / 128.0))
    rest = count - 128.0 * power
    code = (1.0 + rest * (1.0 / 128.0)) * SMALLEST
    power = power.astype(jnp.int32)
    for bit in (0, 1, 2, 3, 4, 5, 6, 7, 7):
        code = jnp.where((power & (1 << bit)) != 0, code * 2.0 ** min(1 << bit, 64), code)
    return jnp.where(value < 0, -code, code).astype(BF)


def decoded(code, top):
    code = code.astype(F32)
    size = jnp.abs(code)
    big = size >= 4.0
    power = jnp.where(big, 128.0, 0.0)
    for _ in range(2):
        size = jnp.where(big, size * 2.0**-64, size)
    for bit in range(6, -1, -1):
        span = float(1 << bit)
        big = size >= SMALLEST * 2.0**span
        size = jnp.where(big, size * 2.0**-span, size)
        power = jnp.where(big, power + span, power)
    count = 128.0 * power + (size * (1.0 / SMALLEST) - 1.0) * 128.0
    return jnp.where(code < 0, -count, count) * (top * (1.0 / STEPS))


def near_body(in_ref, out_ref):
    total = jnp.sum(in_ref[...].astype(F32), axis=0)
    chunk = total.shape[0]
    top = jnp.max(jnp.max(jnp.abs(total), axis=0, keepdims=True), axis=1, keepdims=True)
    top = jnp.maximum(top * 1.0078125, 1e-30).astype(BF)
    code = coded(total, top.astype(F32))
    head = jnp.broadcast_to(top, (8, LANES))
    for k in range(out_ref.shape[0]):
        out_ref[k, :chunk, :] = code
        out_ref[k, chunk:, :] = head


def far_body(in_ref, out_ref):
    chunk = out_ref.shape[1]
    total = None
    for k in range(in_ref.shape[0]):
        top = in_ref[k, chunk:, :].astype(F32)[:1]
        term = decoded(in_ref[k, :chunk, :], top)
        total = term if total is None else total + term
    out_ref[...] = jnp.broadcast_to(total.astype(BF)[None], out_ref.shape)


def unpack_body(scale, in_ref, out_ref, whole, sem):
    chans = out_ref.shape[-1]
    step = chans + chans // 2
    copies = []
    for t in range(9):
        base = t * step
        near = in_ref[base : base + chans, :].astype(F32) * scale
        far = in_ref[base + chans : base + step, :].astype(F32) * scale
        whole[t, :, :LANES] = near
        whole[t, : chans // 2, LANES:] = far[:, : LANES // 2]
        whole[t, chans // 2 :, LANES:] = pltpu.roll(far, LANES // 2, 1)[:, : LANES // 2]
        copy = pltpu.make_async_copy(whole.at[t], out_ref.at[t], sem.at[t])
        copy.start()
        copies.append(copy)
    for copy in copies:
        copy.wait()


def input_body(pair_ref, below_ref, weight_ref, out_ref):
    rows, _, width = out_ref.shape
    half = rows // 2
    grads = [pair_ref[k, 0] for k in range(half)] + [below_ref[0]]
    moved = [pair_ref[k, 1] for k in range(half)] + [below_ref[1]]
    here = jnp.concatenate(grads[:half], axis=1)
    right = jnp.concatenate(moved[:half], axis=1)
    here_down = jnp.concatenate(grads[1:], axis=1)
    right_down = jnp.concatenate(moved[1:], axis=1)

    def tap(a, b, g):
        return mm(weight_ref[a, b], g, NN)

    even_even = tap(1, 1, here)
    even_odd = tap(1, 2, here) + tap(1, 0, right)
    odd_even = tap(2, 1, here) + tap(0, 1, here_down)
    odd_odd = tap(2, 2, here) + tap(2, 0, right) + tap(0, 2, here_down) + tap(0, 0, right_down)
    q = lax.broadcasted_iota(jnp.int32, (width, width), 1)
    n = lax.broadcasted_iota(jnp.int32, (width, width), 0)
    target = jnp.where(n < LANES, 2 * n, 2 * (n - LANES) + 1)
    merge = jnp.where(q == target, 1.0, 0.0).astype(BF)
    for k in range(half):
        cut = slice(k * LANES, (k + 1) * LANES)
        for p, left, odd in ((2 * k, even_even, even_odd), (2 * k + 1, odd_even, odd_odd)):
            both = jnp.concatenate([left[:, cut], odd[:, cut]], axis=1).astype(BF)
            out_ref[p] = mm(both, merge, NN).astype(BF)


def shape(dims, dtype):
    return jax.ShapeDtypeStruct(dims, dtype)


def moved_rows(x, by):
    devices = lax.axis_size(ROWS)
    pairs = [(i, i + by) for i in range(devices) if 0 <= i + by < devices]
    return lax.ppermute(x, ROWS, pairs)


def swap(x, axes):
    return lax.all_to_all(x, axes, split_axis=0, concat_axis=0, tiled=True)


def step(grad_out, inputs, weight):
    chans = weight.shape[2]
    rows, cols = inputs.shape[:2]
    half = rows // 2
    near, far = lax.axis_size(NEAR), lax.axis_size(FAR)
    own = TOTAL // lax.axis_size(CORE)
    chunk = own // near
    positions = half * lax.axis_size(ROWS) * (cols // 2) * lax.axis_size(COLS)
    grad = jnp.transpose(grad_out, (0, 2, 1))[0]
    lines = jnp.transpose(inputs, (0, 2, 1))

    sent = call(send_body, shape((lax.axis_size(COLS), chans + 8, LANES), BF), 10**8, 5 * 10**5)(grad)
    got = swap(sent, COLS)
    last, split = call(
        split_body, (shape((chans, cols), BF), shape((rows, chans, cols), BF)), 2 * 10**8, 2 * 10**6
    )(lines)
    above = moved_rows(last, 1)
    terms, pairs = call(
        filter_body,
        (shape((2, own, LANES), F32), shape((half, 2, chans, LANES), BF)),
        10**9,
        4 * 10**6,
    )(got, split, above)
    other = lax.ppermute(terms[1], CORE, [(0, 1), (1, 0)])
    part = call(pair_body, shape((own, LANES), BF), 10**6, 2 * 10**6)(terms, other)
    part, pairs = lax.optimization_barrier((part, pairs))
    below = moved_rows(pairs[0], -1)
    part = swap(part.reshape(near, chunk, LANES), NEAR)
    part = call(near_body, shape((far, chunk + 8, LANES), BF), 10**6, 10**6)(part)
    part, pairs = lax.optimization_barrier((part, pairs))
    part = swap(part, FAR)
    input_grad = call(input_body, shape((rows, chans, cols), BF), 10**9, 2 * 10**6)(pairs, below, weight)
    part, input_grad = lax.optimization_barrier((part, input_grad))
    part = call(far_body, shape((near, chunk, LANES), BF), 10**6, 10**6)(part)
    part = swap(part, NEAR).reshape(own, LANES)
    whole = lax.all_gather(part, CORE, axis=0, tiled=True)
    filter_grad = pl.pallas_call(
        functools.partial(unpack_body, 1.0 / math.sqrt(positions)),
        out_shape=shape((9, chans, chans), F32),
        out_specs=pl.BlockSpec(memory_space=pltpu.HBM),
        scratch_shapes=[pltpu.VMEM((9, chans, chans), F32), pltpu.SemaphoreType.DMA((9,))],
        cost_estimate=pl.CostEstimate(flops=10**6, bytes_accessed=2 * 10**6, transcendentals=0),
        compiler_params=pltpu.CompilerParams(vmem_limit_bytes=24 * 1024 * 1024),
    )(whole)
    return (jnp.transpose(input_grad, (0, 2, 1)), filter_grad.reshape(3, 3, chans, chans))


def solution(mesh):
    split = Mesh(mesh.devices.reshape(2, 4, 8, 2, 2, 2), AXES)
    return build(split)


def build(split):
    return jax.shard_map(
        step,
        mesh=split,
        in_specs=(P(ROWS + COLS, None, None), P(ROWS, COLS, None), P()),
        out_specs=(P(ROWS, COLS, None), P()),
        check_vma=False,
    )
```

```python
import functools
import math

import jax
import jax.numpy as jnp
from jax import lax
from jax.experimental import pallas as pl
from jax.experimental.pallas import tpu as pltpu
from jax.sharding import Mesh
from jax.sharding import PartitionSpec as P


AXES = ("r0", "r1", "z1", "z0", "c0", "c1")
ROWS = ("r0", "r1", "z1", "z0")
COLS = ("c0", "c1")
NEAR = ("r0", "r1", "z0", "c0")
FAR = "z1"
CORE = "c1"
BF = jnp.bfloat16
F32 = jnp.float32
LANES = 128
TOTAL = 3072
NT = (((1,), (1,)), ((), ()))
TN = (((0,), (0,)), ((), ()))
STEPS = 32256.0
SMALLEST = 2.0**-126
NN = (((1,), (0,)), ((), ()))


def mm(a, b, dims):
    return lax.dot_general(a, b, dims, preferred_element_type=F32)


def call(body, outs, flops, moved):
    return pl.pallas_call(
        body,
        out_shape=outs,
        cost_estimate=pl.CostEstimate(flops=flops, bytes_accessed=moved, transcendentals=0),
        compiler_params=pltpu.CompilerParams(vmem_limit_bytes=24 * 1024 * 1024),
    )


def split_matrix(width):
    half = width // 2
    q = lax.broadcasted_iota(jnp.int32, (width, width), 0)
    n = lax.broadcasted_iota(jnp.int32, (width, width), 1)
    source = jnp.where(n < half, 2 * n, 2 * (n - half) + 1)
    return jnp.where(q == source, 1.0, 0.0).astype(BF)


def send_body(grad_ref, out_ref):
    chans, width = grad_ref.shape
    blocks = out_ref.shape[0]
    block = width // blocks
    r = lax.broadcasted_iota(jnp.int32, (8, width), 0)
    q = lax.broadcasted_iota(jnp.int32, (8, width), 1)
    pick = jnp.where(q == (r + 1) * block, 1.0, 0.0).astype(BF)
    edge = mm(pick, grad_ref[...], NT)
    head = edge[:, :LANES].astype(BF)
    tail = jnp.concatenate([edge[:, LANES:], jnp.zeros((8, 2 * LANES - chans), F32)], axis=1).astype(BF)
    for d in range(blocks):
        out_ref[d, :chans, :] = grad_ref[:, d * block : (d + 1) * block]
        out_ref[d, chans:, :] = jnp.concatenate(
            [head[d : d + 1], tail[d : d + 1], jnp.zeros((6, LANES), BF)], axis=0
        )


def split_body(lines_ref, split_ref):
    rows, chans, width = lines_ref.shape
    flat = lines_ref[...].reshape(rows * chans, width)
    split_ref[...] = mm(flat, split_matrix(width), NN).astype(BF).reshape(rows, chans, width)


def shifted(grads, edges):
    q = lax.broadcasted_iota(jnp.int32, (LANES, LANES), 0)
    n = lax.broadcasted_iota(jnp.int32, (LANES, LANES), 1)
    move = jnp.where(q == n + 1, 1.0, 0.0).astype(BF)
    r = lax.broadcasted_iota(jnp.int32, (8, LANES), 0)
    lane = lax.broadcasted_iota(jnp.int32, (8, LANES), 1)
    out = []
    for k, block in enumerate(grads):
        place = jnp.where((r == k) & (lane == LANES - 1), 1.0, 0.0).astype(BF)
        out.append((mm(block, move, NN) + mm(edges, place, TN)).astype(BF))
    return out


def edges_of(blocks, chans):
    rows = [jnp.concatenate([b[chans : chans + 1, :], b[chans + 1 : chans + 2, : chans - LANES]], axis=1) for b in blocks]
    rows.append(jnp.zeros((8 - len(rows), chans), BF))
    return jnp.concatenate(rows, axis=0)


def filter_body(got_ref, split_ref, above_ref, out_ref, pair_ref):
    rows, chans, width = split_ref.shape
    half = rows // 2
    mine = lax.axis_index(CORE)
    top = mm(above_ref[...], split_matrix(width), NN).astype(BF)
    blocks = [got_ref[k] for k in range(half)]
    grads = [b[:chans, :] for b in blocks]
    moved = shifted(grads, edges_of(blocks, chans))
    for k in range(half):
        pair_ref[k, 0] = grads[k]
        pair_ref[k, 1] = moved[k]
    spare = jnp.zeros((2 * LANES - chans, half * LANES), BF)
    here = jnp.concatenate([jnp.concatenate(grads, axis=1), spare], axis=0)
    right = jnp.concatenate([jnp.concatenate(moved, axis=1), spare], axis=0)

    def line(p, odd):
        lanes = slice(LANES, 2 * LANES) if odd else slice(0, LANES)
        return top[:, lanes] if p < 0 else split_ref[p, :, lanes]

    own = out_ref.shape[1]

    def put(base, value):
        count = value.shape[0]
        for core in range(2):
            low, high = max(base, core * own), min(base + count, (core + 1) * own)
            if low < high:
                out_ref[mine ^ core, low - core * own : high - core * own, :] = value[low - base : high - base]

    step = chans + chans // 2
    for a in range(3):
        for b in range(3):
            left = jnp.concatenate([line(2 * k + a - 1, b != 1) for k in range(half)], axis=1)
            term = mm(left, right if b == 0 else here, NT)
            base = (3 * a + b) * step
            far = term[:, LANES:]
            put(base, term[:, :LANES])
            put(base + chans, far[: chans // 2] + pltpu.roll(far[chans // 2 :], LANES // 2, 1))
    put(9 * step, jnp.zeros((TOTAL - 9 * step, LANES), F32))


def pair_body(mine_ref, other_ref, out_ref):
    out_ref[...] = (mine_ref[0] + other_ref[...]).astype(BF)


def coded(value, top):
    count = jnp.floor(jnp.abs(value) * (STEPS / top) + 0.5)
    power = jnp.floor(count * (1.0 / 128.0))
    rest = count - 128.0 * power
    code = (1.0 + rest * (1.0 / 128.0)) * SMALLEST
    power = power.astype(jnp.int32)
    for bit in (0, 1, 2, 3, 4, 5, 6, 7, 7):
        code = jnp.where((power & (1 << bit)) != 0, code * 2.0 ** min(1 << bit, 64), code)
    return jnp.where(value < 0, -code, code).astype(BF)


def decoded(code, top):
    code = code.astype(F32)
    size = jnp.abs(code)
    big = size >= 4.0
    power = jnp.where(big, 128.0, 0.0)
    for _ in range(2):
        size = jnp.where(big, size * 2.0**-64, size)
    for bit in range(6, -1, -1):
        span = float(1 << bit)
        big = size >= SMALLEST * 2.0**span
        size = jnp.where(big, size * 2.0**-span, size)
        power = jnp.where(big, power + span, power)
    count = 128.0 * power + (size * (1.0 / SMALLEST) - 1.0) * 128.0
    return jnp.where(code < 0, -count, count) * (top * (1.0 / STEPS))


def near_body(in_ref, out_ref):
    total = jnp.sum(in_ref[...].astype(F32), axis=0)
    chunk = total.shape[0]
    top = jnp.max(jnp.max(jnp.abs(total), axis=0, keepdims=True), axis=1, keepdims=True)
    top = jnp.maximum(top * 1.0078125, 1e-30).astype(BF)
    code = coded(total, top.astype(F32))
    head = jnp.broadcast_to(top, (8, LANES))
    for k in range(out_ref.shape[0]):
        out_ref[k, :chunk, :] = code
        out_ref[k, chunk:, :] = head


def far_body(in_ref, out_ref):
    chunk = out_ref.shape[1]
    total = None
    for k in range(in_ref.shape[0]):
        top = in_ref[k, chunk:, :].astype(F32)[:1]
        term = decoded(in_ref[k, :chunk, :], top)
        total = term if total is None else total + term
    out_ref[...] = jnp.broadcast_to(total.astype(BF)[None], out_ref.shape)


def unpack_body(scale, in_ref, out_ref, whole, sem):
    chans = out_ref.shape[-1]
    step = chans + chans // 2
    copies = []
    for t in range(9):
        base = t * step
        near = in_ref[base : base + chans, :].astype(F32) * scale
        far = in_ref[base + chans : base + step, :].astype(F32) * scale
        whole[t, :, :LANES] = near
        whole[t, : chans // 2, LANES:] = far[:, : LANES // 2]
        whole[t, chans // 2 :, LANES:] = pltpu.roll(far, LANES // 2, 1)[:, : LANES // 2]
        copy = pltpu.make_async_copy(whole.at[t], out_ref.at[t], sem.at[t])
        copy.start()
        copies.append(copy)
    for copy in copies:
        copy.wait()


def input_body(pair_ref, below_ref, weight_ref, out_ref):
    rows, _, width = out_ref.shape
    half = rows // 2
    grads = [pair_ref[k, 0] for k in range(half)] + [below_ref[0]]
    moved = [pair_ref[k, 1] for k in range(half)] + [below_ref[1]]
    here = jnp.concatenate(grads[:half], axis=1)
    right = jnp.concatenate(moved[:half], axis=1)
    here_down = jnp.concatenate(grads[1:], axis=1)
    right_down = jnp.concatenate(moved[1:], axis=1)

    def tap(a, b, g):
        return mm(weight_ref[a, b], g, NN)

    even_even = tap(1, 1, here)
    even_odd = tap(1, 2, here) + tap(1, 0, right)
    odd_even = tap(2, 1, here) + tap(0, 1, here_down)
    odd_odd = tap(2, 2, here) + tap(2, 0, right) + tap(0, 2, here_down) + tap(0, 0, right_down)
    q = lax.broadcasted_iota(jnp.int32, (width, width), 1)
    n = lax.broadcasted_iota(jnp.int32, (width, width), 0)
    target = jnp.where(n < LANES, 2 * n, 2 * (n - LANES) + 1)
    merge = jnp.where(q == target, 1.0, 0.0).astype(BF)
    for k in range(half):
        cut = slice(k * LANES, (k + 1) * LANES)
        for p, left, odd in ((2 * k, even_even, even_odd), (2 * k + 1, odd_even, odd_odd)):
            both = jnp.concatenate([left[:, cut], odd[:, cut]], axis=1).astype(BF)
            out_ref[p] = mm(both, merge, NN).astype(BF)


def shape(dims, dtype):
    return jax.ShapeDtypeStruct(dims, dtype)


def moved_rows(x, by):
    devices = lax.axis_size(ROWS)
    pairs = [(i, i + by) for i in range(devices) if 0 <= i + by < devices]
    return lax.ppermute(x, ROWS, pairs)


def swap(x, axes):
    return lax.all_to_all(x, axes, split_axis=0, concat_axis=0, tiled=True)


def step(grad_out, inputs, weight):
    chans = weight.shape[2]
    rows, cols = inputs.shape[:2]
    half = rows // 2
    near, far = lax.axis_size(NEAR), lax.axis_size(FAR)
    own = TOTAL // lax.axis_size(CORE)
    chunk = own // near
    positions = half * lax.axis_size(ROWS) * (cols // 2) * lax.axis_size(COLS)
    grad = jnp.transpose(grad_out, (0, 2, 1))[0]
    lines = jnp.transpose(inputs, (0, 2, 1))

    sent = call(send_body, shape((lax.axis_size(COLS), chans + 8, LANES), BF), 10**8, 5 * 10**5)(grad)
    got = swap(sent, COLS)
    above = moved_rows(lines[rows - 1], 1)
    split = call(split_body, shape((rows, chans, cols), BF), 2 * 10**8, 2 * 10**6)(lines)
    terms, pairs = call(
        filter_body,
        (shape((2, own, LANES), F32), shape((half, 2, chans, LANES), BF)),
        10**9,
        4 * 10**6,
    )(got, split, above)
    other = lax.ppermute(terms[1], CORE, [(0, 1), (1, 0)])
    below = moved_rows(pairs[0], -1)
    part = call(pair_body, shape((own, LANES), BF), 10**6, 2 * 10**6)(terms, other)
    part = swap(part.reshape(near, chunk, LANES), NEAR)
    part = call(near_body, shape((far, chunk + 8, LANES), BF), 10**6, 10**6)(part)
    part, pairs = lax.optimization_barrier((part, pairs))
    part = swap(part, FAR)
    input_grad = call(input_body, shape((rows, chans, cols), BF), 10**9, 2 * 10**6)(pairs, below, weight)
    part, input_grad = lax.optimization_barrier((part, input_grad))
    part = call(far_body, shape((near, chunk, LANES), BF), 10**6, 10**6)(part)
    part = swap(part, NEAR).reshape(own, LANES)
    whole = lax.all_gather(part, CORE, axis=0, tiled=True)
    filter_grad = pl.pallas_call(
        functools.partial(unpack_body, 1.0 / math.sqrt(positions)),
        out_shape=shape((9, chans, chans), F32),
        out_specs=pl.BlockSpec(memory_space=pltpu.HBM),
        scratch_shapes=[pltpu.VMEM((9, chans, chans), F32), pltpu.SemaphoreType.DMA((9,))],
        cost_estimate=pl.CostEstimate(flops=10**6, bytes_accessed=2 * 10**6, transcendentals=0),
        compiler_params=pltpu.CompilerParams(vmem_limit_bytes=24 * 1024 * 1024),
    )(whole)
    return (jnp.transpose(input_grad, (0, 2, 1)), filter_grad.reshape(3, 3, chans, chans))


def solution(mesh):
    split = Mesh(mesh.devices.reshape(2, 4, 8, 2, 2, 2), AXES)
    return build(split)


def build(split):
    return jax.shard_map(
        step,
        mesh=split,
        in_specs=(P(ROWS + COLS, None, None), P(ROWS, COLS, None), P()),
        out_specs=(P(ROWS, COLS, None), P()),
        check_vma=False,
    )
```

```python
import functools
import math

import jax
import jax.numpy as jnp
from jax import lax
from jax.experimental import pallas as pl
from jax.experimental.pallas import tpu as pltpu
from jax.sharding import Mesh
from jax.sharding import PartitionSpec as P


AXES = ("r0", "r1", "z1", "z0", "c0", "c1")
ROWS = ("r0", "r1", "z1", "z0")
COLS = ("c0", "c1")
NEAR = ("r0", "r1", "z0", "c0")
FAR = "z1"
CORE = "c1"
BF = jnp.bfloat16
F32 = jnp.float32
LANES = 128
TOTAL = 3072
NT = (((1,), (1,)), ((), ()))
TN = (((0,), (0,)), ((), ()))
STEPS = 32256.0
SMALLEST = 2.0**-126
NN = (((1,), (0,)), ((), ()))


def mm(a, b, dims):
    return lax.dot_general(a, b, dims, preferred_element_type=F32)


def call(body, outs, flops, moved):
    return pl.pallas_call(
        body,
        out_shape=outs,
        cost_estimate=pl.CostEstimate(flops=flops, bytes_accessed=moved, transcendentals=0),
        compiler_params=pltpu.CompilerParams(vmem_limit_bytes=24 * 1024 * 1024),
    )


def split_matrix(width):
    half = width // 2
    q = lax.broadcasted_iota(jnp.int32, (width, width), 0)
    n = lax.broadcasted_iota(jnp.int32, (width, width), 1)
    source = jnp.where(n < half, 2 * n, 2 * (n - half) + 1)
    return jnp.where(q == source, 1.0, 0.0).astype(BF)


def send_body(grad_ref, line_ref, out_ref, row_ref):
    chans, width = grad_ref.shape
    row_ref[...] = line_ref[0]
    blocks = out_ref.shape[0]
    block = width // blocks
    r = lax.broadcasted_iota(jnp.int32, (8, width), 0)
    q = lax.broadcasted_iota(jnp.int32, (8, width), 1)
    pick = jnp.where(q == (r + 1) * block, 1.0, 0.0).astype(BF)
    edge = mm(pick, grad_ref[...], NT)
    head = edge[:, :LANES].astype(BF)
    tail = jnp.concatenate([edge[:, LANES:], jnp.zeros((8, 2 * LANES - chans), F32)], axis=1).astype(BF)
    for d in range(blocks):
        out_ref[d, :chans, :] = grad_ref[:, d * block : (d + 1) * block]
        out_ref[d, chans:, :] = jnp.concatenate(
            [head[d : d + 1], tail[d : d + 1], jnp.zeros((6, LANES), BF)], axis=0
        )


def split_body(lines_ref, split_ref):
    rows, chans, width = lines_ref.shape
    flat = lines_ref[...].reshape(rows * chans, width)
    split_ref[...] = mm(flat, split_matrix(width), NN).astype(BF).reshape(rows, chans, width)


def shifted(grads, edges):
    q = lax.broadcasted_iota(jnp.int32, (LANES, LANES), 0)
    n = lax.broadcasted_iota(jnp.int32, (LANES, LANES), 1)
    move = jnp.where(q == n + 1, 1.0, 0.0).astype(BF)
    r = lax.broadcasted_iota(jnp.int32, (8, LANES), 0)
    lane = lax.broadcasted_iota(jnp.int32, (8, LANES), 1)
    out = []
    for k, block in enumerate(grads):
        place = jnp.where((r == k) & (lane == LANES - 1), 1.0, 0.0).astype(BF)
        out.append((mm(block, move, NN) + mm(edges, place, TN)).astype(BF))
    return out


def edges_of(blocks, chans):
    rows = [jnp.concatenate([b[chans : chans + 1, :], b[chans + 1 : chans + 2, : chans - LANES]], axis=1) for b in blocks]
    rows.append(jnp.zeros((8 - len(rows), chans), BF))
    return jnp.concatenate(rows, axis=0)


def filter_body(got_ref, split_ref, above_ref, out_ref, pair_ref):
    rows, chans, width = split_ref.shape
    half = rows // 2
    mine = lax.axis_index(CORE)
    top = mm(above_ref[...], split_matrix(width), NN).astype(BF)
    blocks = [got_ref[k] for k in range(half)]
    grads = [b[:chans, :] for b in blocks]
    moved = shifted(grads, edges_of(blocks, chans))
    for k in range(half):
        pair_ref[k, 0] = grads[k]
        pair_ref[k, 1] = moved[k]
    spare = jnp.zeros((2 * LANES - chans, half * LANES), BF)
    here = jnp.concatenate([jnp.concatenate(grads, axis=1), spare], axis=0)
    right = jnp.concatenate([jnp.concatenate(moved, axis=1), spare], axis=0)

    def line(p, odd):
        lanes = slice(LANES, 2 * LANES) if odd else slice(0, LANES)
        return top[:, lanes] if p < 0 else split_ref[p, :, lanes]

    own = out_ref.shape[1]

    def put(base, value):
        count = value.shape[0]
        for core in range(2):
            low, high = max(base, core * own), min(base + count, (core + 1) * own)
            if low < high:
                out_ref[mine ^ core, low - core * own : high - core * own, :] = value[low - base : high - base]

    step = chans + chans // 2
    for a in range(3):
        for b in range(3):
            left = jnp.concatenate([line(2 * k + a - 1, b != 1) for k in range(half)], axis=1)
            term = mm(left, right if b == 0 else here, NT)
            base = (3 * a + b) * step
            far = term[:, LANES:]
            put(base, term[:, :LANES])
            put(base + chans, far[: chans // 2] + pltpu.roll(far[chans // 2 :], LANES // 2, 1))
    put(9 * step, jnp.zeros((TOTAL - 9 * step, LANES), F32))


def pair_body(mine_ref, other_ref, out_ref):
    out_ref[...] = (mine_ref[0] + other_ref[...]).astype(BF)


def coded(value, top):
    count = jnp.floor(jnp.abs(value) * (STEPS / top) + 0.5)
    power = jnp.floor(count * (1.0 / 128.0))
    rest = count - 128.0 * power
    code = (1.0 + rest * (1.0 / 128.0)) * SMALLEST
    power = power.astype(jnp.int32)
    for bit in (0, 1, 2, 3, 4, 5, 6, 7, 7):
        code = jnp.where((power & (1 << bit)) != 0, code * 2.0 ** min(1 << bit, 64), code)
    return jnp.where(value < 0, -code, code).astype(BF)


def decoded(code, top):
    code = code.astype(F32)
    size = jnp.abs(code)
    big = size >= 4.0
    power = jnp.where(big, 128.0, 0.0)
    for _ in range(2):
        size = jnp.where(big, size * 2.0**-64, size)
    for bit in range(6, -1, -1):
        span = float(1 << bit)
        big = size >= SMALLEST * 2.0**span
        size = jnp.where(big, size * 2.0**-span, size)
        power = jnp.where(big, power + span, power)
    count = 128.0 * power + (size * (1.0 / SMALLEST) - 1.0) * 128.0
    return jnp.where(code < 0, -count, count) * (top * (1.0 / STEPS))


def near_body(in_ref, out_ref):
    total = jnp.sum(in_ref[...].astype(F32), axis=0)
    chunk = total.shape[0]
    top = jnp.max(jnp.max(jnp.abs(total), axis=0, keepdims=True), axis=1, keepdims=True)
    top = jnp.maximum(top * 1.0078125, 1e-30).astype(BF)
    code = coded(total, top.astype(F32))
    head = jnp.broadcast_to(top, (8, LANES))
    for k in range(out_ref.shape[0]):
        out_ref[k, :chunk, :] = code
        out_ref[k, chunk:, :] = head


def far_body(in_ref, out_ref):
    chunk = out_ref.shape[1]
    total = None
    for k in range(in_ref.shape[0]):
        top = in_ref[k, chunk:, :].astype(F32)[:1]
        term = decoded(in_ref[k, :chunk, :], top)
        total = term if total is None else total + term
    out_ref[...] = jnp.broadcast_to(total.astype(BF)[None], out_ref.shape)


def unpack_body(scale, in_ref, out_ref, whole, sem):
    chans = out_ref.shape[-1]
    step = chans + chans // 2
    copies = []
    for t in range(9):
        base = t * step
        near = in_ref[base : base + chans, :].astype(F32) * scale
        far = in_ref[base + chans : base + step, :].astype(F32) * scale
        whole[t, :, :LANES] = near
        whole[t, : chans // 2, LANES:] = far[:, : LANES // 2]
        whole[t, chans // 2 :, LANES:] = pltpu.roll(far, LANES // 2, 1)[:, : LANES // 2]
        copy = pltpu.make_async_copy(whole.at[t], out_ref.at[t], sem.at[t])
        copy.start()
        copies.append(copy)
    for copy in copies:
        copy.wait()


def input_body(pair_ref, below_ref, weight_ref, out_ref):
    rows, _, width = out_ref.shape
    half = rows // 2
    grads = [pair_ref[k, 0] for k in range(half)] + [below_ref[0]]
    moved = [pair_ref[k, 1] for k in range(half)] + [below_ref[1]]
    here = jnp.concatenate(grads[:half], axis=1)
    right = jnp.concatenate(moved[:half], axis=1)
    here_down = jnp.concatenate(grads[1:], axis=1)
    right_down = jnp.concatenate(moved[1:], axis=1)

    def tap(a, b, g):
        return mm(weight_ref[a, b], g, NN)

    even_even = tap(1, 1, here)
    even_odd = tap(1, 2, here) + tap(1, 0, right)
    odd_even = tap(2, 1, here) + tap(0, 1, here_down)
    odd_odd = tap(2, 2, here) + tap(2, 0, right) + tap(0, 2, here_down) + tap(0, 0, right_down)
    q = lax.broadcasted_iota(jnp.int32, (width, width), 1)
    n = lax.broadcasted_iota(jnp.int32, (width, width), 0)
    target = jnp.where(n < LANES, 2 * n, 2 * (n - LANES) + 1)
    merge = jnp.where(q == target, 1.0, 0.0).astype(BF)
    for k in range(half):
        cut = slice(k * LANES, (k + 1) * LANES)
        for p, left, odd in ((2 * k, even_even, even_odd), (2 * k + 1, odd_even, odd_odd)):
            both = jnp.concatenate([left[:, cut], odd[:, cut]], axis=1).astype(BF)
            out_ref[p] = mm(both, merge, NN).astype(BF)


def shape(dims, dtype):
    return jax.ShapeDtypeStruct(dims, dtype)


def moved_rows(x, by):
    devices = lax.axis_size(ROWS)
    pairs = [(i, i + by) for i in range(devices) if 0 <= i + by < devices]
    return lax.ppermute(x, ROWS, pairs)


def swap(x, axes):
    return lax.all_to_all(x, axes, split_axis=0, concat_axis=0, tiled=True)


def step(grad_out, inputs, weight):
    chans = weight.shape[2]
    rows, cols = inputs.shape[:2]
    half = rows // 2
    near, far = lax.axis_size(NEAR), lax.axis_size(FAR)
    own = TOTAL // lax.axis_size(CORE)
    chunk = own // near
    positions = half * lax.axis_size(ROWS) * (cols // 2) * lax.axis_size(COLS)
    grad = jnp.transpose(grad_out, (0, 2, 1))[0]
    lines = jnp.transpose(inputs, (0, 2, 1))

    sent, last = pl.pallas_call(
        send_body,
        grid=(1,),
        in_specs=[
            pl.BlockSpec(grad.shape, lambda i: (0, 0)),
            pl.BlockSpec((1, chans, cols), lambda i: (rows - 1, 0, 0)),
        ],
        out_specs=[
            pl.BlockSpec((lax.axis_size(COLS), chans + 8, LANES), lambda i: (0, 0, 0)),
            pl.BlockSpec((chans, cols), lambda i: (0, 0)),
        ],
        out_shape=[shape((lax.axis_size(COLS), chans + 8, LANES), BF), shape((chans, cols), BF)],
        cost_estimate=pl.CostEstimate(flops=10**8, bytes_accessed=5 * 10**5, transcendentals=0),
        compiler_params=pltpu.CompilerParams(vmem_limit_bytes=63000000),
    )(grad, lines)
    got = swap(sent, COLS)
    above = moved_rows(last, 1)
    split = call(split_body, shape((rows, chans, cols), BF), 2 * 10**8, 2 * 10**6)(lines)
    terms, pairs = call(
        filter_body,
        (shape((2, own, LANES), F32), shape((half, 2, chans, LANES), BF)),
        10**9,
        4 * 10**6,
    )(got, split, above)
    other = lax.ppermute(terms[1], CORE, [(0, 1), (1, 0)])
    part = call(pair_body, shape((own, LANES), BF), 10**6, 2 * 10**6)(terms, other)
    part = swap(part.reshape(near, chunk, LANES), NEAR)
    part = call(near_body, shape((far, chunk + 8, LANES), BF), 10**6, 10**6)(part)
    part, pairs = lax.optimization_barrier((part, pairs))
    part = swap(part, FAR)
    below = moved_rows(pairs[0], -1)
    part = call(far_body, shape((near, chunk, LANES), BF), 10**6, 10**6)(part)
    part = swap(part, NEAR).reshape(own, LANES)
    input_grad = call(input_body, shape((rows, chans, cols), BF), 10**9, 2 * 10**6)(pairs, below, weight)
    part, input_grad = lax.optimization_barrier((part, input_grad))
    whole = lax.all_gather(part, CORE, axis=0, tiled=True)
    filter_grad = pl.pallas_call(
        functools.partial(unpack_body, 1.0 / math.sqrt(positions)),
        out_shape=shape((9, chans, chans), F32),
        out_specs=pl.BlockSpec(memory_space=pltpu.HBM),
        scratch_shapes=[pltpu.VMEM((9, chans, chans), F32), pltpu.SemaphoreType.DMA((9,))],
        cost_estimate=pl.CostEstimate(flops=10**6, bytes_accessed=2 * 10**6, transcendentals=0),
        compiler_params=pltpu.CompilerParams(vmem_limit_bytes=24 * 1024 * 1024),
    )(whole)
    return (jnp.transpose(input_grad, (0, 2, 1)), filter_grad.reshape(3, 3, chans, chans))


def solution(mesh):
    split = Mesh(mesh.devices.reshape(2, 4, 8, 2, 2, 2), AXES)
    return build(split)


def build(split):
    return jax.shard_map(
        step,
        mesh=split,
        in_specs=(P(ROWS + COLS, None, None), P(ROWS, COLS, None), P()),
        out_specs=(P(ROWS, COLS, None), P()),
        check_vma=False,
    )
```

```python
import functools
import math

import jax
import jax.numpy as jnp
from jax import lax
from jax.experimental import pallas as pl
from jax.experimental.pallas import tpu as pltpu
from jax.sharding import Mesh
from jax.sharding import PartitionSpec as P


AXES = ("r0", "r1", "z1", "z0", "c0", "c1")
ROWS = ("r0", "r1", "z1", "z0")
COLS = ("c0", "c1")
NEAR = ("r0", "r1", "z0", "c0")
FAR = "z1"
CORE = "c1"
BF = jnp.bfloat16
F32 = jnp.float32
LANES = 128
TOTAL = 3072
NT = (((1,), (1,)), ((), ()))
TN = (((0,), (0,)), ((), ()))
STEPS = 32256.0
SMALLEST = 2.0**-126
NN = (((1,), (0,)), ((), ()))


def mm(a, b, dims):
    return lax.dot_general(a, b, dims, preferred_element_type=F32)


def call(body, outs, flops, moved):
    return pl.pallas_call(
        body,
        out_shape=outs,
        cost_estimate=pl.CostEstimate(flops=flops, bytes_accessed=moved, transcendentals=0),
        compiler_params=pltpu.CompilerParams(vmem_limit_bytes=24 * 1024 * 1024),
    )


def split_matrix(width):
    half = width // 2
    q = lax.broadcasted_iota(jnp.int32, (width, width), 0)
    n = lax.broadcasted_iota(jnp.int32, (width, width), 1)
    source = jnp.where(n < half, 2 * n, 2 * (n - half) + 1)
    return jnp.where(q == source, 1.0, 0.0).astype(BF)


def send_body(grad_ref, line_ref, out_ref, row_ref):
    chans, width = grad_ref.shape
    row_ref[...] = line_ref[0]
    blocks = out_ref.shape[0]
    block = width // blocks
    r = lax.broadcasted_iota(jnp.int32, (8, width), 0)
    q = lax.broadcasted_iota(jnp.int32, (8, width), 1)
    pick = jnp.where(q == (r + 1) * block, 1.0, 0.0).astype(BF)
    edge = mm(pick, grad_ref[...], NT)
    head = edge[:, :LANES].astype(BF)
    tail = jnp.concatenate([edge[:, LANES:], jnp.zeros((8, 2 * LANES - chans), F32)], axis=1).astype(BF)
    for d in range(blocks):
        out_ref[d, :chans, :] = grad_ref[:, d * block : (d + 1) * block]
        out_ref[d, chans:, :] = jnp.concatenate(
            [head[d : d + 1], tail[d : d + 1], jnp.zeros((6, LANES), BF)], axis=0
        )


def split_body(lines_ref, split_ref):
    rows, chans, width = lines_ref.shape
    flat = lines_ref[...].reshape(rows * chans, width)
    split_ref[...] = mm(flat, split_matrix(width), NN).astype(BF).reshape(rows, chans, width)


def shifted(grads, edges):
    q = lax.broadcasted_iota(jnp.int32, (LANES, LANES), 0)
    n = lax.broadcasted_iota(jnp.int32, (LANES, LANES), 1)
    move = jnp.where(q == n + 1, 1.0, 0.0).astype(BF)
    r = lax.broadcasted_iota(jnp.int32, (8, LANES), 0)
    lane = lax.broadcasted_iota(jnp.int32, (8, LANES), 1)
    out = []
    for k, block in enumerate(grads):
        place = jnp.where((r == k) & (lane == LANES - 1), 1.0, 0.0).astype(BF)
        out.append((mm(block, move, NN) + mm(edges, place, TN)).astype(BF))
    return out


def edges_of(blocks, chans):
    rows = [jnp.concatenate([b[chans : chans + 1, :], b[chans + 1 : chans + 2, : chans - LANES]], axis=1) for b in blocks]
    rows.append(jnp.zeros((8 - len(rows), chans), BF))
    return jnp.concatenate(rows, axis=0)


def filter_body(got_ref, split_ref, above_ref, out_ref, pair_ref):
    rows, chans, width = split_ref.shape
    half = rows // 2
    mine = lax.axis_index(CORE)
    top = mm(above_ref[...], split_matrix(width), NN).astype(BF)
    blocks = [got_ref[k] for k in range(half)]
    grads = [b[:chans, :] for b in blocks]
    moved = shifted(grads, edges_of(blocks, chans))
    for k in range(half):
        pair_ref[k, 0] = grads[k]
        pair_ref[k, 1] = moved[k]
    spare = jnp.zeros((2 * LANES - chans, half * LANES), BF)
    here = jnp.concatenate([jnp.concatenate(grads, axis=1), spare], axis=0)
    right = jnp.concatenate([jnp.concatenate(moved, axis=1), spare], axis=0)

    def line(p, odd):
        lanes = slice(LANES, 2 * LANES) if odd else slice(0, LANES)
        return top[:, lanes] if p < 0 else split_ref[p, :, lanes]

    own = out_ref.shape[1]

    def put(base, value):
        count = value.shape[0]
        for core in range(2):
            low, high = max(base, core * own), min(base + count, (core + 1) * own)
            if low < high:
                out_ref[mine ^ core, low - core * own : high - core * own, :] = value[low - base : high - base]

    step = chans + chans // 2
    for a in range(3):
        for b in range(3):
            left = jnp.concatenate([line(2 * k + a - 1, b != 1) for k in range(half)], axis=1)
            term = mm(left, right if b == 0 else here, NT)
            base = (3 * a + b) * step
            far = term[:, LANES:]
            put(base, term[:, :LANES])
            put(base + chans, far[: chans // 2] + pltpu.roll(far[chans // 2 :], LANES // 2, 1))
    put(9 * step, jnp.zeros((TOTAL - 9 * step, LANES), F32))


def pair_body(mine_ref, other_ref, out_ref):
    out_ref[...] = (mine_ref[0] + other_ref[...]).astype(BF)


def coded(value, top):
    count = jnp.floor(jnp.abs(value) * (STEPS / top) + 0.5)
    power = jnp.floor(count * (1.0 / 128.0))
    rest = count - 128.0 * power
    code = (1.0 + rest * (1.0 / 128.0)) * SMALLEST
    power = power.astype(jnp.int32)
    for bit in (0, 1, 2, 3, 4, 5, 6, 7, 7):
        code = jnp.where((power & (1 << bit)) != 0, code * 2.0 ** min(1 << bit, 64), code)
    return jnp.where(value < 0, -code, code).astype(BF)


def decoded(code, top):
    code = code.astype(F32)
    size = jnp.abs(code)
    big = size >= 4.0
    power = jnp.where(big, 128.0, 0.0)
    for _ in range(2):
        size = jnp.where(big, size * 2.0**-64, size)
    for bit in range(6, -1, -1):
        span = float(1 << bit)
        big = size >= SMALLEST * 2.0**span
        size = jnp.where(big, size * 2.0**-span, size)
        power = jnp.where(big, power + span, power)
    count = 128.0 * power + (size * (1.0 / SMALLEST) - 1.0) * 128.0
    return jnp.where(code < 0, -count, count) * (top * (1.0 / STEPS))


def near_body(in_ref, out_ref):
    total = jnp.sum(in_ref[...].astype(F32), axis=0)
    chunk = total.shape[0]
    top = jnp.max(jnp.max(jnp.abs(total), axis=0, keepdims=True), axis=1, keepdims=True)
    top = jnp.maximum(top * 1.0078125, 1e-30).astype(BF)
    code = coded(total, top.astype(F32))
    head = jnp.broadcast_to(top, (8, LANES))
    for k in range(out_ref.shape[0]):
        out_ref[k, :chunk, :] = code
        out_ref[k, chunk:, :] = head


def far_body(in_ref, out_ref):
    chunk = out_ref.shape[1]
    total = None
    for k in range(in_ref.shape[0]):
        top = in_ref[k, chunk:, :].astype(F32)[:1]
        term = decoded(in_ref[k, :chunk, :], top)
        total = term if total is None else total + term
    out_ref[...] = jnp.broadcast_to(total.astype(BF)[None], out_ref.shape)


def merge_matrix(width):
    half = width // 2
    n = lax.broadcasted_iota(jnp.int32, (width, width), 0)
    q = lax.broadcasted_iota(jnp.int32, (width, width), 1)
    return jnp.where(q == jnp.where(n < half, 2 * n, 2 * (n - half) + 1), 1.0, 0.0).astype(BF)


def merged(even, odd, merge):
    return mm(jnp.concatenate([even, odd], axis=1).astype(BF), merge, NN).astype(BF)


def input_body(pair_ref, weight_ref, out_ref, part_ref):
    rows, chans, width = out_ref.shape
    half = rows // 2
    grads = [pair_ref[k, 0] for k in range(half)]
    moved = [pair_ref[k, 1] for k in range(half)]
    here = jnp.concatenate(grads, axis=1)
    right = jnp.concatenate(moved, axis=1)
    here_down = jnp.concatenate(grads[1:], axis=1)
    right_down = jnp.concatenate(moved[1:], axis=1)

    def tap(a, b, g):
        return mm(weight_ref[a, b], g, NN)

    even_even = tap(1, 1, here)
    even_odd = tap(1, 2, here) + tap(1, 0, right)
    odd_even = tap(2, 1, here)
    odd_odd = tap(2, 2, here) + tap(2, 0, right)
    odd_even_down = tap(0, 1, here_down)
    odd_odd_down = tap(0, 2, here_down) + tap(0, 0, right_down)
    merge = merge_matrix(width)
    for k in range(half):
        cut = slice(k * LANES, (k + 1) * LANES)
        out_ref[2 * k] = merged(even_even[:, cut], even_odd[:, cut], merge)
        if k < half - 1:
            out_ref[2 * k + 1] = merged(
                odd_even[:, cut] + odd_even_down[:, cut], odd_odd[:, cut] + odd_odd_down[:, cut], merge
            )
        else:
            part_ref[0] = odd_even[:, cut]
            part_ref[1] = odd_odd[:, cut]
            out_ref[2 * k + 1] = jnp.zeros((chans, width), BF)


def last_body(scale, in_ref, below_ref, weight_ref, part_ref, _, out_ref, grad_ref, whole, line, sem):
    chans = out_ref.shape[-1]
    rows, _, width = grad_ref.shape
    step = chans + chans // 2
    copies = []
    for t in range(9):
        base = t * step
        near = in_ref[base : base + chans, :].astype(F32) * scale
        far = in_ref[base + chans : base + step, :].astype(F32) * scale
        whole[t, :, :LANES] = near
        whole[t, : chans // 2, LANES:] = far[:, : LANES // 2]
        whole[t, chans // 2 :, LANES:] = pltpu.roll(far, LANES // 2, 1)[:, : LANES // 2]
        copy = pltpu.make_async_copy(whole.at[t], out_ref.at[t], sem.at[t])
        copy.start()
        copies.append(copy)
    block = below_ref[...]
    here = block[:chans, :]
    right = shifted([here], edges_of([block], chans))[0]
    even = part_ref[0] + mm(weight_ref[0, 1], here, NN)
    odd = part_ref[1] + mm(weight_ref[0, 2], here, NN) + mm(weight_ref[0, 0], right, NN)
    line[...] = merged(even, odd, merge_matrix(width))
    copy = pltpu.make_async_copy(line, grad_ref.at[rows - 1], sem.at[9])
    copy.start()
    copies.append(copy)
    for copy in copies:
        copy.wait()


def shape(dims, dtype):
    return jax.ShapeDtypeStruct(dims, dtype)


def moved_rows(x, by):
    devices = lax.axis_size(ROWS)
    pairs = [(i, i + by) for i in range(devices) if 0 <= i + by < devices]
    return lax.ppermute(x, ROWS, pairs)


def swap(x, axes):
    return lax.all_to_all(x, axes, split_axis=0, concat_axis=0, tiled=True)


def step(grad_out, inputs, weight):
    chans = weight.shape[2]
    rows, cols = inputs.shape[:2]
    half = rows // 2
    near, far = lax.axis_size(NEAR), lax.axis_size(FAR)
    own = TOTAL // lax.axis_size(CORE)
    chunk = own // near
    positions = half * lax.axis_size(ROWS) * (cols // 2) * lax.axis_size(COLS)
    grad = jnp.transpose(grad_out, (0, 2, 1))[0]
    lines = jnp.transpose(inputs, (0, 2, 1))

    sent, last = pl.pallas_call(
        send_body,
        grid=(1,),
        in_specs=[
            pl.BlockSpec(grad.shape, lambda i: (0, 0)),
            pl.BlockSpec((1, chans, cols), lambda i: (rows - 1, 0, 0)),
        ],
        out_specs=[
            pl.BlockSpec((lax.axis_size(COLS), chans + 8, LANES), lambda i: (0, 0, 0)),
            pl.BlockSpec((chans, cols), lambda i: (0, 0)),
        ],
        out_shape=[shape((lax.axis_size(COLS), chans + 8, LANES), BF), shape((chans, cols), BF)],
        cost_estimate=pl.CostEstimate(flops=10**8, bytes_accessed=5 * 10**5, transcendentals=0),
        compiler_params=pltpu.CompilerParams(vmem_limit_bytes=63000000),
    )(grad, lines)
    got = swap(sent, COLS)
    above = moved_rows(last, 1)
    split = call(split_body, shape((rows, chans, cols), BF), 2 * 10**8, 2 * 10**6)(lines)
    below = moved_rows(got[0], -1)
    terms, pairs = call(
        filter_body,
        (shape((2, own, LANES), F32), shape((half, 2, chans, LANES), BF)),
        10**9,
        4 * 10**6,
    )(got, split, above)
    other = lax.ppermute(terms[1], CORE, [(0, 1), (1, 0)])
    input_grad, odd_part = call(
        input_body, (shape((rows, chans, cols), BF), shape((2, chans, LANES), F32)), 10**9, 2 * 10**6
    )(pairs, weight)
    part = call(pair_body, shape((own, LANES), BF), 10**6, 2 * 10**6)(terms, other)
    part = swap(part.reshape(near, chunk, LANES), NEAR)
    part = call(near_body, shape((far, chunk + 8, LANES), BF), 10**6, 10**6)(part)
    part = swap(part, FAR)
    part = call(far_body, shape((near, chunk, LANES), BF), 10**6, 10**6)(part)
    part = swap(part, NEAR).reshape(own, LANES)
    whole = lax.all_gather(part, CORE, axis=0, tiled=True)
    stored = pl.BlockSpec(memory_space=pltpu.HBM)
    local = pl.BlockSpec(memory_space=pltpu.VMEM)
    filter_grad, input_grad = pl.pallas_call(
        functools.partial(last_body, 1.0 / math.sqrt(positions)),
        out_shape=(shape((9, chans, chans), F32), shape((rows, chans, cols), BF)),
        in_specs=[local, local, local, local, stored],
        out_specs=(stored, stored),
        input_output_aliases={4: 1},
        scratch_shapes=[
            pltpu.VMEM((9, chans, chans), F32),
            pltpu.VMEM((chans, cols), BF),
            pltpu.SemaphoreType.DMA((10,)),
        ],
        cost_estimate=pl.CostEstimate(flops=10**6, bytes_accessed=2 * 10**6, transcendentals=0),
        compiler_params=pltpu.CompilerParams(vmem_limit_bytes=24 * 1024 * 1024),
    )(whole, below, weight, odd_part, input_grad)
    return (jnp.transpose(input_grad, (0, 2, 1)), filter_grad.reshape(3, 3, chans, chans))


def solution(mesh):
    split = Mesh(mesh.devices.reshape(2, 4, 8, 2, 2, 2), AXES)
    return build(split)


def build(split):
    return jax.shard_map(
        step,
        mesh=split,
        in_specs=(P(ROWS + COLS, None, None), P(ROWS, COLS, None), P()),
        out_specs=(P(ROWS, COLS, None), P()),
        check_vma=False,
    )
```

```python
import functools
import math

import jax
import jax.numpy as jnp
from jax import lax
from jax.experimental import pallas as pl
from jax.experimental.pallas import tpu as pltpu
from jax.sharding import Mesh
from jax.sharding import PartitionSpec as P


AXES = ("r0", "r1", "z1", "z0", "c0", "c1")
ROWS = ("r0", "r1", "z1", "z0")
COLS = ("c0", "c1")
NEAR = ("r0", "r1", "z0", "c0")
FAR = "z1"
CORE = "c1"
BF = jnp.bfloat16
F32 = jnp.float32
LANES = 128
TOTAL = 3072
NT = (((1,), (1,)), ((), ()))
TN = (((0,), (0,)), ((), ()))
STEPS = 32256.0
SMALLEST = 2.0**-126
NN = (((1,), (0,)), ((), ()))


def mm(a, b, dims):
    return lax.dot_general(a, b, dims, preferred_element_type=F32)


def call(body, outs, flops, moved):
    return pl.pallas_call(
        body,
        out_shape=outs,
        cost_estimate=pl.CostEstimate(flops=flops, bytes_accessed=moved, transcendentals=0),
        compiler_params=pltpu.CompilerParams(vmem_limit_bytes=24 * 1024 * 1024),
    )


def split_matrix(width):
    half = width // 2
    q = lax.broadcasted_iota(jnp.int32, (width, width), 0)
    n = lax.broadcasted_iota(jnp.int32, (width, width), 1)
    source = jnp.where(n < half, 2 * n, 2 * (n - half) + 1)
    return jnp.where(q == source, 1.0, 0.0).astype(BF)


def send_body(grad_ref, lines_ref, out_ref, row_ref, grad, line, edges, in_sem, out_sem):
    chans, width = grad_ref.shape
    blocks = out_ref.shape[0]
    block = width // blocks
    take_grad = pltpu.make_async_copy(grad_ref, grad, in_sem.at[0])
    take_line = pltpu.make_async_copy(lines_ref.at[lines_ref.shape[0] - 1], line, in_sem.at[1])
    take_grad.start()
    take_line.start()
    r = lax.broadcasted_iota(jnp.int32, (8, width), 0)
    q = lax.broadcasted_iota(jnp.int32, (8, width), 1)
    pick = jnp.where(q == (r + 1) * block, 1.0, 0.0).astype(BF)
    take_grad.wait()
    puts = []
    for d in range(blocks):
        puts.append(
            pltpu.make_async_copy(
                grad.at[:, pl.ds(d * block, block)], out_ref.at[d, pl.ds(0, chans), :], out_sem.at[d]
            )
        )
    puts.append(pltpu.make_async_copy(line, row_ref, out_sem.at[blocks]))
    for put in puts[:blocks]:
        put.start()
    edge = mm(pick, grad[...], NT)
    head = edge[:, :LANES]
    tail = jnp.concatenate([edge[:, LANES:], jnp.zeros((8, 2 * LANES - chans), F32)], axis=1)
    take_line.wait()
    puts[blocks].start()
    for d in range(blocks):
        edges[d] = jnp.concatenate([head[d : d + 1], tail[d : d + 1], jnp.zeros((6, LANES), F32)], axis=0).astype(BF)
    puts.append(pltpu.make_async_copy(edges, out_ref.at[:, pl.ds(chans, 8), :], out_sem.at[blocks + 1]))
    puts[-1].start()
    for put in puts:
        put.wait()


def split_body(lines_ref, split_ref):
    rows, chans, width = lines_ref.shape
    flat = lines_ref[...].reshape(rows * chans, width)
    split_ref[...] = mm(flat, split_matrix(width), NN).astype(BF).reshape(rows, chans, width)


def shifted(grads, edges):
    q = lax.broadcasted_iota(jnp.int32, (LANES, LANES), 0)
    n = lax.broadcasted_iota(jnp.int32, (LANES, LANES), 1)
    move = jnp.where(q == n + 1, 1.0, 0.0).astype(BF)
    r = lax.broadcasted_iota(jnp.int32, (8, LANES), 0)
    lane = lax.broadcasted_iota(jnp.int32, (8, LANES), 1)
    out = []
    for k, block in enumerate(grads):
        place = jnp.where((r == k) & (lane == LANES - 1), 1.0, 0.0).astype(BF)
        out.append((mm(block, move, NN) + mm(edges, place, TN)).astype(BF))
    return out


def edges_of(blocks, chans):
    rows = [jnp.concatenate([b[chans : chans + 1, :], b[chans + 1 : chans + 2, : chans - LANES]], axis=1) for b in blocks]
    rows.append(jnp.zeros((8 - len(rows), chans), BF))
    return jnp.concatenate(rows, axis=0)


def filter_body(got_ref, split_ref, above_ref, out_ref, pair_ref):
    rows, chans, width = split_ref.shape
    half = rows // 2
    mine = lax.axis_index(CORE)
    top = mm(above_ref[...], split_matrix(width), NN).astype(BF)
    blocks = [got_ref[k] for k in range(half)]
    grads = [b[:chans, :] for b in blocks]
    moved = shifted(grads, edges_of(blocks, chans))
    for k in range(half):
        pair_ref[k, 0] = grads[k]
        pair_ref[k, 1] = moved[k]
    spare = jnp.zeros((2 * LANES - chans, half * LANES), BF)
    here = jnp.concatenate([jnp.concatenate(grads, axis=1), spare], axis=0)
    right = jnp.concatenate([jnp.concatenate(moved, axis=1), spare], axis=0)

    def line(p, odd):
        lanes = slice(LANES, 2 * LANES) if odd else slice(0, LANES)
        return top[:, lanes] if p < 0 else split_ref[p, :, lanes]

    own = out_ref.shape[1]

    def put(base, value):
        count = value.shape[0]
        for core in range(2):
            low, high = max(base, core * own), min(base + count, (core + 1) * own)
            if low < high:
                out_ref[mine ^ core, low - core * own : high - core * own, :] = value[low - base : high - base]

    step = chans + chans // 2
    for a in range(3):
        for b in range(3):
            left = jnp.concatenate([line(2 * k + a - 1, b != 1) for k in range(half)], axis=1)
            term = mm(left, right if b == 0 else here, NT)
            base = (3 * a + b) * step
            far = term[:, LANES:]
            put(base, term[:, :LANES])
            put(base + chans, far[: chans // 2] + pltpu.roll(far[chans // 2 :], LANES // 2, 1))
    put(9 * step, jnp.zeros((TOTAL - 9 * step, LANES), F32))


def pair_body(mine_ref, other_ref, out_ref):
    out_ref[...] = (mine_ref[0] + other_ref[...]).astype(BF)


def coded(value, top):
    count = jnp.floor(jnp.abs(value) * (STEPS / top) + 0.5)
    power = jnp.floor(count * (1.0 / 128.0))
    rest = count - 128.0 * power
    code = (1.0 + rest * (1.0 / 128.0)) * SMALLEST
    power = power.astype(jnp.int32)
    for bit in (0, 1, 2, 3, 4, 5, 6, 7, 7):
        code = jnp.where((power & (1 << bit)) != 0, code * 2.0 ** min(1 << bit, 64), code)
    return jnp.where(value < 0, -code, code).astype(BF)


def decoded(code, top):
    code = code.astype(F32)
    size = jnp.abs(code)
    big = size >= 4.0
    power = jnp.where(big, 128.0, 0.0)
    for _ in range(2):
        size = jnp.where(big, size * 2.0**-64, size)
    for bit in range(6, -1, -1):
        span = float(1 << bit)
        big = size >= SMALLEST * 2.0**span
        size = jnp.where(big, size * 2.0**-span, size)
        power = jnp.where(big, power + span, power)
    count = 128.0 * power + (size * (1.0 / SMALLEST) - 1.0) * 128.0
    return jnp.where(code < 0, -count, count) * (top * (1.0 / STEPS))


def near_body(in_ref, out_ref):
    total = jnp.sum(in_ref[...].astype(F32), axis=0)
    chunk = total.shape[0]
    top = jnp.max(jnp.max(jnp.abs(total), axis=0, keepdims=True), axis=1, keepdims=True)
    top = jnp.maximum(top * 1.0078125, 1e-30).astype(BF)
    code = coded(total, top.astype(F32))
    head = jnp.broadcast_to(top, (8, LANES))
    for k in range(out_ref.shape[0]):
        out_ref[k, :chunk, :] = code
        out_ref[k, chunk:, :] = head


def far_body(in_ref, out_ref):
    chunk = out_ref.shape[1]
    total = None
    for k in range(in_ref.shape[0]):
        top = in_ref[k, chunk:, :].astype(F32)[:1]
        term = decoded(in_ref[k, :chunk, :], top)
        total = term if total is None else total + term
    out_ref[...] = jnp.broadcast_to(total.astype(BF)[None], out_ref.shape)


def merge_matrix(width):
    half = width // 2
    n = lax.broadcasted_iota(jnp.int32, (width, width), 0)
    q = lax.broadcasted_iota(jnp.int32, (width, width), 1)
    return jnp.where(q == jnp.where(n < half, 2 * n, 2 * (n - half) + 1), 1.0, 0.0).astype(BF)


def merged(even, odd, merge):
    return mm(jnp.concatenate([even, odd], axis=1).astype(BF), merge, NN).astype(BF)


def input_body(pair_ref, weight_ref, out_ref, part_ref):
    rows, chans, width = out_ref.shape
    half = rows // 2
    grads = [pair_ref[k, 0] for k in range(half)]
    moved = [pair_ref[k, 1] for k in range(half)]
    here = jnp.concatenate(grads, axis=1)
    right = jnp.concatenate(moved, axis=1)
    here_down = jnp.concatenate(grads[1:], axis=1)
    right_down = jnp.concatenate(moved[1:], axis=1)

    def tap(a, b, g):
        return mm(weight_ref[a, b], g, NN)

    even_even = tap(1, 1, here)
    even_odd = tap(1, 2, here) + tap(1, 0, right)
    odd_even = tap(2, 1, here)
    odd_odd = tap(2, 2, here) + tap(2, 0, right)
    odd_even_down = tap(0, 1, here_down)
    odd_odd_down = tap(0, 2, here_down) + tap(0, 0, right_down)
    merge = merge_matrix(width)
    for k in range(half):
        cut = slice(k * LANES, (k + 1) * LANES)
        out_ref[2 * k] = merged(even_even[:, cut], even_odd[:, cut], merge)
        if k < half - 1:
            out_ref[2 * k + 1] = merged(
                odd_even[:, cut] + odd_even_down[:, cut], odd_odd[:, cut] + odd_odd_down[:, cut], merge
            )
        else:
            part_ref[0] = odd_even[:, cut]
            part_ref[1] = odd_odd[:, cut]
            out_ref[2 * k + 1] = jnp.zeros((chans, width), BF)


def last_body(scale, in_ref, below_ref, weight_ref, part_ref, _, out_ref, grad_ref, whole, line, sem):
    chans = out_ref.shape[-1]
    rows, _, width = grad_ref.shape
    step = chans + chans // 2
    copies = []

    def tap(t):
        base = t * step
        near = in_ref[base : base + chans, :].astype(F32) * scale
        far = in_ref[base + chans : base + step, :].astype(F32) * scale
        whole[t, :, :LANES] = near
        whole[t, : chans // 2, LANES:] = far[:, : LANES // 2]
        whole[t, chans // 2 :, LANES:] = pltpu.roll(far, LANES // 2, 1)[:, : LANES // 2]
        copies.append(pltpu.make_async_copy(whole.at[t], out_ref.at[t], sem.at[t]))
        copies[-1].start()

    for t in range(3):
        tap(t)
    block = below_ref[...]
    here = block[:chans, :]
    right = shifted([here], edges_of([block], chans))[0]
    even = part_ref[0] + mm(weight_ref[0, 1], here, NN)
    odd = part_ref[1] + mm(weight_ref[0, 2], here, NN) + mm(weight_ref[0, 0], right, NN)
    line[...] = merged(even, odd, merge_matrix(width))
    copies.append(pltpu.make_async_copy(line, grad_ref.at[rows - 1], sem.at[9]))
    copies[-1].start()
    for t in range(3, 9):
        tap(t)
    for copy in copies:
        copy.wait()


def shape(dims, dtype):
    return jax.ShapeDtypeStruct(dims, dtype)


def moved_rows(x, by):
    devices = lax.axis_size(ROWS)
    pairs = [(i, i + by) for i in range(devices) if 0 <= i + by < devices]
    return lax.ppermute(x, ROWS, pairs)


def swap(x, axes):
    return lax.all_to_all(x, axes, split_axis=0, concat_axis=0, tiled=True)


def step(grad_out, inputs, weight):
    chans = weight.shape[2]
    rows, cols = inputs.shape[:2]
    half = rows // 2
    near, far = lax.axis_size(NEAR), lax.axis_size(FAR)
    own = TOTAL // lax.axis_size(CORE)
    chunk = own // near
    positions = half * lax.axis_size(ROWS) * (cols // 2) * lax.axis_size(COLS)
    grad = jnp.transpose(grad_out, (0, 2, 1))[0]
    lines = jnp.transpose(inputs, (0, 2, 1))

    stored = pl.BlockSpec(memory_space=pltpu.HBM)
    local = pl.BlockSpec(memory_space=pltpu.VMEM)
    blocks = lax.axis_size(COLS)
    sent, last = pl.pallas_call(
        send_body,
        in_specs=[stored, stored],
        out_specs=[stored, stored],
        out_shape=[shape((blocks, chans + 8, LANES), BF), shape((chans, cols), BF)],
        scratch_shapes=[
            pltpu.VMEM(grad.shape, BF),
            pltpu.VMEM((chans, cols), BF),
            pltpu.VMEM((blocks, 8, LANES), BF),
            pltpu.SemaphoreType.DMA((2,)),
            pltpu.SemaphoreType.DMA((blocks + 2,)),
        ],
        cost_estimate=pl.CostEstimate(flops=10**8, bytes_accessed=5 * 10**5, transcendentals=0),
        compiler_params=pltpu.CompilerParams(vmem_limit_bytes=63000000),
    )(grad, lines)
    got = swap(sent, COLS)
    above = moved_rows(last, 1)
    split = call(split_body, shape((rows, chans, cols), BF), 2 * 10**8, 2 * 10**6)(lines)
    below = moved_rows(got[0], -1)
    terms, pairs = call(
        filter_body,
        (shape((2, own, LANES), F32), shape((half, 2, chans, LANES), BF)),
        10**9,
        4 * 10**6,
    )(got, split, above)
    other = lax.ppermute(terms[1], CORE, [(0, 1), (1, 0)])
    input_grad, odd_part = call(
        input_body, (shape((rows, chans, cols), BF), shape((2, chans, LANES), F32)), 10**9, 2 * 10**6
    )(pairs, weight)
    part = call(pair_body, shape((own, LANES), BF), 10**6, 2 * 10**6)(terms, other)
    part = swap(part.reshape(near, chunk, LANES), NEAR)
    part = call(near_body, shape((far, chunk + 8, LANES), BF), 10**6, 10**6)(part)
    part = lax.all_to_all(part, FAR, 0, 0, tiled=True, axis_index_groups=[[4, 5, 6, 7, 0, 1, 2, 3]])
    part = call(far_body, shape((near, chunk, LANES), BF), 10**6, 10**6)(part)
    part = swap(part, NEAR).reshape(own, LANES)
    whole = lax.all_gather(part, CORE, axis=0, tiled=True)
    filter_grad, input_grad = pl.pallas_call(
        functools.partial(last_body, 1.0 / math.sqrt(positions)),
        out_shape=(shape((9, chans, chans), F32), shape((rows, chans, cols), BF)),
        in_specs=[local, local, local, local, stored],
        out_specs=(stored, stored),
        input_output_aliases={4: 1},
        scratch_shapes=[
            pltpu.VMEM((9, chans, chans), F32),
            pltpu.VMEM((chans, cols), BF),
            pltpu.SemaphoreType.DMA((10,)),
        ],
        cost_estimate=pl.CostEstimate(flops=10**6, bytes_accessed=2 * 10**6, transcendentals=0),
        compiler_params=pltpu.CompilerParams(vmem_limit_bytes=24 * 1024 * 1024),
    )(whole, below, weight, odd_part, input_grad)
    return (jnp.transpose(input_grad, (0, 2, 1)), filter_grad.reshape(3, 3, chans, chans))


def solution(mesh):
    split = Mesh(mesh.devices.reshape(2, 4, 8, 2, 2, 2), AXES)
    return build(split)


def build(split):
    return jax.shard_map(
        step,
        mesh=split,
        in_specs=(P(ROWS + COLS, None, None), P(ROWS, COLS, None), P()),
        out_specs=(P(ROWS, COLS, None), P()),
        check_vma=False,
    )
```

```python
import functools
import itertools
import math

import jax
import jax.numpy as jnp
from jax import lax
from jax.experimental import pallas as pl
from jax.experimental.pallas import tpu as pltpu
from jax.sharding import Mesh
from jax.sharding import PartitionSpec as P


AXES = ("r0", "r1", "z1", "z0", "c0", "c1")
ROWS = ("r0", "r1", "z1", "z0")
COLS = ("c0", "c1")
NEAR = ("r0", "r1", "z0", "c0")
FAR = "z1"
CORE = "c1"
OPEN_COLS = (0, 1)
OPEN_FIRST = (0, 2, 0, 1)
OPEN_THIRD = (0, 2, 0, 1)
OPEN_FAR = (5,)
BF = jnp.bfloat16
F32 = jnp.float32
LANES = 128
TOTAL = 3072
NT = (((1,), (1,)), ((), ()))
TN = (((0,), (0,)), ((), ()))
STEPS = 32256.0
SMALLEST = 2.0**-126
NN = (((1,), (0,)), ((), ()))


def mm(a, b, dims):
    return lax.dot_general(a, b, dims, preferred_element_type=F32)


def call(body, outs, flops, moved):
    return pl.pallas_call(
        body,
        out_shape=outs,
        cost_estimate=pl.CostEstimate(flops=flops, bytes_accessed=moved, transcendentals=0),
        compiler_params=pltpu.CompilerParams(vmem_limit_bytes=24 * 1024 * 1024),
    )


def split_matrix(width):
    half = width // 2
    q = lax.broadcasted_iota(jnp.int32, (width, width), 0)
    n = lax.broadcasted_iota(jnp.int32, (width, width), 1)
    source = jnp.where(n < half, 2 * n, 2 * (n - half) + 1)
    return jnp.where(q == source, 1.0, 0.0).astype(BF)


def send_body(order, grad_ref, lines_ref, out_ref, row_ref, grad, line, edges, in_sem, out_sem):
    chans, width = grad_ref.shape
    blocks = out_ref.shape[0]
    block = width // blocks
    take_grad = pltpu.make_async_copy(grad_ref, grad, in_sem.at[0])
    take_line = pltpu.make_async_copy(lines_ref.at[lines_ref.shape[0] - 1], line, in_sem.at[1])
    take_grad.start()
    take_line.start()
    r = lax.broadcasted_iota(jnp.int32, (8, width), 0)
    q = lax.broadcasted_iota(jnp.int32, (8, width), 1)
    pick = jnp.where(q == (r + 1) * block, 1.0, 0.0).astype(BF)
    take_grad.wait()
    puts = []
    for d in range(blocks):
        puts.append(
            pltpu.make_async_copy(
                grad.at[:, pl.ds(order[d] * block, block)], out_ref.at[d, pl.ds(0, chans), :], out_sem.at[d]
            )
        )
    puts.append(pltpu.make_async_copy(line, row_ref, out_sem.at[blocks]))
    for put in puts[:blocks]:
        put.start()
    edge = mm(pick, grad[...], NT)
    head = edge[:, :LANES]
    tail = jnp.concatenate([edge[:, LANES:], jnp.zeros((8, 2 * LANES - chans), F32)], axis=1)
    take_line.wait()
    puts[blocks].start()
    for d in range(blocks):
        k = order[d]
        edges[d] = jnp.concatenate([head[k : k + 1], tail[k : k + 1], jnp.zeros((6, LANES), F32)], axis=0).astype(BF)
    puts.append(pltpu.make_async_copy(edges, out_ref.at[:, pl.ds(chans, 8), :], out_sem.at[blocks + 1]))
    puts[-1].start()
    for put in puts:
        put.wait()


def split_body(lines_ref, split_ref):
    rows, chans, width = lines_ref.shape
    flat = lines_ref[...].reshape(rows * chans, width)
    split_ref[...] = mm(flat, split_matrix(width), NN).astype(BF).reshape(rows, chans, width)


def shifted(grads, edges):
    q = lax.broadcasted_iota(jnp.int32, (LANES, LANES), 0)
    n = lax.broadcasted_iota(jnp.int32, (LANES, LANES), 1)
    move = jnp.where(q == n + 1, 1.0, 0.0).astype(BF)
    r = lax.broadcasted_iota(jnp.int32, (8, LANES), 0)
    lane = lax.broadcasted_iota(jnp.int32, (8, LANES), 1)
    out = []
    for k, block in enumerate(grads):
        place = jnp.where((r == k) & (lane == LANES - 1), 1.0, 0.0).astype(BF)
        out.append((mm(block, move, NN) + mm(edges, place, TN)).astype(BF))
    return out


def edges_of(blocks, chans):
    rows = [jnp.concatenate([b[chans : chans + 1, :], b[chans + 1 : chans + 2, : chans - LANES]], axis=1) for b in blocks]
    rows.append(jnp.zeros((8 - len(rows), chans), BF))
    return jnp.concatenate(rows, axis=0)


def filter_body(order, got_ref, split_ref, above_ref, out_ref, pair_ref):
    rows, chans, width = split_ref.shape
    half = rows // 2
    mine = lax.axis_index(CORE)
    top = mm(above_ref[...], split_matrix(width), NN).astype(BF)
    blocks = [got_ref[order.index(k)] for k in range(half)]
    grads = [b[:chans, :] for b in blocks]
    moved = shifted(grads, edges_of(blocks, chans))
    for k in range(half):
        pair_ref[k, 0] = grads[k]
        pair_ref[k, 1] = moved[k]
    spare = jnp.zeros((2 * LANES - chans, half * LANES), BF)
    here = jnp.concatenate([jnp.concatenate(grads, axis=1), spare], axis=0)
    right = jnp.concatenate([jnp.concatenate(moved, axis=1), spare], axis=0)

    def line(p, odd):
        lanes = slice(LANES, 2 * LANES) if odd else slice(0, LANES)
        return top[:, lanes] if p < 0 else split_ref[p, :, lanes]

    own = out_ref.shape[1]

    def put(base, value):
        count = value.shape[0]
        for core in range(2):
            low, high = max(base, core * own), min(base + count, (core + 1) * own)
            if low < high:
                out_ref[mine ^ core, low - core * own : high - core * own, :] = value[low - base : high - base]

    step = chans + chans // 2
    for a in range(3):
        for b in range(3):
            left = jnp.concatenate([line(2 * k + a - 1, b != 1) for k in range(half)], axis=1)
            term = mm(left, right if b == 0 else here, NT)
            base = (3 * a + b) * step
            far = term[:, LANES:]
            put(base, term[:, :LANES])
            put(base + chans, far[: chans // 2] + pltpu.roll(far[chans // 2 :], LANES // 2, 1))
    put(9 * step, jnp.zeros((TOTAL - 9 * step, LANES), F32))


def pair_body(sources, mine_ref, other_ref, out_ref):
    chunk = out_ref.shape[0] // len(sources)
    for place, source in enumerate(sources):
        rows = slice(source * chunk, (source + 1) * chunk)
        out_ref[place * chunk : (place + 1) * chunk, :] = (mine_ref[0, rows, :] + other_ref[rows, :]).astype(BF)


def coded(value, top):
    count = jnp.floor(jnp.abs(value) * (STEPS / top) + 0.5)
    power = jnp.floor(count * (1.0 / 128.0))
    rest = count - 128.0 * power
    code = (1.0 + rest * (1.0 / 128.0)) * SMALLEST
    power = power.astype(jnp.int32)
    for bit in (0, 1, 2, 3, 4, 5, 6, 7, 7):
        code = jnp.where((power & (1 << bit)) != 0, code * 2.0 ** min(1 << bit, 64), code)
    return jnp.where(value < 0, -code, code).astype(BF)


def decoded(code, top):
    code = code.astype(F32)
    size = jnp.abs(code)
    big = size >= 4.0
    power = jnp.where(big, 128.0, 0.0)
    for _ in range(2):
        size = jnp.where(big, size * 2.0**-64, size)
    for bit in range(6, -1, -1):
        span = float(1 << bit)
        big = size >= SMALLEST * 2.0**span
        size = jnp.where(big, size * 2.0**-span, size)
        power = jnp.where(big, power + span, power)
    count = 128.0 * power + (size * (1.0 / SMALLEST) - 1.0) * 128.0
    return jnp.where(code < 0, -count, count) * (top * (1.0 / STEPS))


def near_body(in_ref, out_ref):
    total = jnp.sum(in_ref[...].astype(F32), axis=0)
    chunk = total.shape[0]
    top = jnp.max(jnp.max(jnp.abs(total), axis=0, keepdims=True), axis=1, keepdims=True)
    top = jnp.maximum(top * 1.0078125, 1e-30).astype(BF)
    code = coded(total, top.astype(F32))
    head = jnp.broadcast_to(top, (8, LANES))
    for k in range(out_ref.shape[0]):
        out_ref[k, :chunk, :] = code
        out_ref[k, chunk:, :] = head


def far_body(in_ref, out_ref):
    chunk = out_ref.shape[1]
    total = None
    for k in range(in_ref.shape[0]):
        top = in_ref[k, chunk:, :].astype(F32)[:1]
        term = decoded(in_ref[k, :chunk, :], top)
        total = term if total is None else total + term
    out_ref[...] = jnp.broadcast_to(total.astype(BF)[None], out_ref.shape)


def merge_matrix(width):
    half = width // 2
    n = lax.broadcasted_iota(jnp.int32, (width, width), 0)
    q = lax.broadcasted_iota(jnp.int32, (width, width), 1)
    return jnp.where(q == jnp.where(n < half, 2 * n, 2 * (n - half) + 1), 1.0, 0.0).astype(BF)


def merged(even, odd, merge):
    return mm(jnp.concatenate([even, odd], axis=1).astype(BF), merge, NN).astype(BF)


def input_body(pair_ref, weight_ref, out_ref, part_ref):
    rows, chans, width = out_ref.shape
    half = rows // 2
    grads = [pair_ref[k, 0] for k in range(half)]
    moved = [pair_ref[k, 1] for k in range(half)]
    here = jnp.concatenate(grads, axis=1)
    right = jnp.concatenate(moved, axis=1)
    here_down = jnp.concatenate(grads[1:], axis=1)
    right_down = jnp.concatenate(moved[1:], axis=1)

    def tap(a, b, g):
        return mm(weight_ref[a, b], g, NN)

    even_even = tap(1, 1, here)
    even_odd = tap(1, 2, here) + tap(1, 0, right)
    odd_even = tap(2, 1, here)
    odd_odd = tap(2, 2, here) + tap(2, 0, right)
    odd_even_down = tap(0, 1, here_down)
    odd_odd_down = tap(0, 2, here_down) + tap(0, 0, right_down)
    merge = merge_matrix(width)
    for k in range(half):
        cut = slice(k * LANES, (k + 1) * LANES)
        out_ref[2 * k] = merged(even_even[:, cut], even_odd[:, cut], merge)
        if k < half - 1:
            out_ref[2 * k + 1] = merged(
                odd_even[:, cut] + odd_even_down[:, cut], odd_odd[:, cut] + odd_odd_down[:, cut], merge
            )
        else:
            part_ref[0] = odd_even[:, cut]
            part_ref[1] = odd_odd[:, cut]
            out_ref[2 * k + 1] = jnp.zeros((chans, width), BF)


def last_body(scale, in_ref, below_ref, weight_ref, part_ref, _, out_ref, grad_ref, whole, line, sem):
    chans = out_ref.shape[-1]
    rows, _, width = grad_ref.shape
    step = chans + chans // 2
    copies = []

    def tap(t):
        base = t * step
        near = in_ref[base : base + chans, :].astype(F32) * scale
        far = in_ref[base + chans : base + step, :].astype(F32) * scale
        whole[t, :, :LANES] = near
        whole[t, : chans // 2, LANES:] = far[:, : LANES // 2]
        whole[t, chans // 2 :, LANES:] = pltpu.roll(far, LANES // 2, 1)[:, : LANES // 2]
        copies.append(pltpu.make_async_copy(whole.at[t], out_ref.at[t], sem.at[t]))
        copies[-1].start()

    for t in range(3):
        tap(t)
    block = below_ref[...]
    here = block[:chans, :]
    right = shifted([here], edges_of([block], chans))[0]
    even = part_ref[0] + mm(weight_ref[0, 1], here, NN)
    odd = part_ref[1] + mm(weight_ref[0, 2], here, NN) + mm(weight_ref[0, 0], right, NN)
    line[...] = merged(even, odd, merge_matrix(width))
    copies.append(pltpu.make_async_copy(line, grad_ref.at[rows - 1], sem.at[9]))
    copies[-1].start()
    for t in range(3, 9):
        tap(t)
    for copy in copies:
        copy.wait()


def shape(dims, dtype):
    return jax.ShapeDtypeStruct(dims, dtype)


def moved_rows(x, by):
    devices = lax.axis_size(ROWS)
    pairs = [(i, i + by) for i in range(devices) if 0 <= i + by < devices]
    return lax.ppermute(x, ROWS, pairs)


def opened(axes, at):
    sizes = [lax.axis_size(axis) for axis in axes]
    order = []
    for place in itertools.product(*(range(size) for size in sizes)):
        index = 0
        for step, start, size in zip(place, at, sizes):
            index = index * size + (step + start) % size
        order.append(index)
    return order


def swap(x, axes, order):
    return lax.all_to_all(x, axes, split_axis=0, concat_axis=0, tiled=True, axis_index_groups=[order])


def step(grad_out, inputs, weight):
    chans = weight.shape[2]
    rows, cols = inputs.shape[:2]
    half = rows // 2
    near, far = lax.axis_size(NEAR), lax.axis_size(FAR)
    own = TOTAL // lax.axis_size(CORE)
    chunk = own // near
    positions = half * lax.axis_size(ROWS) * (cols // 2) * lax.axis_size(COLS)
    grad = jnp.transpose(grad_out, (0, 2, 1))[0]
    lines = jnp.transpose(inputs, (0, 2, 1))

    stored = pl.BlockSpec(memory_space=pltpu.HBM)
    local = pl.BlockSpec(memory_space=pltpu.VMEM)
    blocks = lax.axis_size(COLS)
    across = opened(COLS, OPEN_COLS)
    first = opened(NEAR, OPEN_FIRST)
    third = opened(NEAR, OPEN_THIRD)
    sent, last = pl.pallas_call(
        functools.partial(send_body, across),
        in_specs=[stored, stored],
        out_specs=[stored, stored],
        out_shape=[shape((blocks, chans + 8, LANES), BF), shape((chans, cols), BF)],
        scratch_shapes=[
            pltpu.VMEM(grad.shape, BF),
            pltpu.VMEM((chans, cols), BF),
            pltpu.VMEM((blocks, 8, LANES), BF),
            pltpu.SemaphoreType.DMA((2,)),
            pltpu.SemaphoreType.DMA((blocks + 2,)),
        ],
        cost_estimate=pl.CostEstimate(flops=10**8, bytes_accessed=5 * 10**5, transcendentals=0),
        compiler_params=pltpu.CompilerParams(vmem_limit_bytes=63000000),
    )(grad, lines)
    got = swap(sent, COLS, across)
    above = moved_rows(last, 1)
    split = call(split_body, shape((rows, chans, cols), BF), 2 * 10**8, 2 * 10**6)(lines)
    below = moved_rows(got[across.index(0)], -1)
    terms, pairs = call(
        functools.partial(filter_body, across),
        (shape((2, own, LANES), F32), shape((half, 2, chans, LANES), BF)),
        10**9,
        4 * 10**6,
    )(got, split, above)
    other = lax.ppermute(terms[1], CORE, [(0, 1), (1, 0)])
    input_grad, odd_part = call(
        input_body, (shape((rows, chans, cols), BF), shape((2, chans, LANES), F32)), 10**9, 2 * 10**6
    )(pairs, weight)
    sources = [third.index(device) for device in first]
    part = call(functools.partial(pair_body, sources), shape((own, LANES), BF), 10**6, 2 * 10**6)(terms, other)
    part = swap(part.reshape(near, chunk, LANES), NEAR, first)
    part = call(near_body, shape((far, chunk + 8, LANES), BF), 10**6, 10**6)(part)
    part = swap(part, FAR, opened((FAR,), OPEN_FAR))
    part = call(far_body, shape((near, chunk, LANES), BF), 10**6, 10**6)(part)
    part = swap(part, NEAR, third).reshape(own, LANES)
    whole = lax.all_gather(part, CORE, axis=0, tiled=True)
    filter_grad, input_grad = pl.pallas_call(
        functools.partial(last_body, 1.0 / math.sqrt(positions)),
        out_shape=(shape((9, chans, chans), F32), shape((rows, chans, cols), BF)),
        in_specs=[local, local, local, local, stored],
        out_specs=(stored, stored),
        input_output_aliases={4: 1},
        scratch_shapes=[
            pltpu.VMEM((9, chans, chans), F32),
            pltpu.VMEM((chans, cols), BF),
            pltpu.SemaphoreType.DMA((10,)),
        ],
        cost_estimate=pl.CostEstimate(flops=10**6, bytes_accessed=2 * 10**6, transcendentals=0),
        compiler_params=pltpu.CompilerParams(vmem_limit_bytes=24 * 1024 * 1024),
    )(whole, below, weight, odd_part, input_grad)
    return (jnp.transpose(input_grad, (0, 2, 1)), filter_grad.reshape(3, 3, chans, chans))


def solution(mesh):
    split = Mesh(mesh.devices.reshape(2, 4, 8, 2, 2, 2), AXES)
    return build(split)


def build(split):
    return jax.shard_map(
        step,
        mesh=split,
        in_specs=(P(ROWS + COLS, None, None), P(ROWS, COLS, None), P()),
        out_specs=(P(ROWS, COLS, None), P()),
        check_vma=False,
    )
```
